128 devices in a mesh: ctx: 32 (over y, x, core), head: 4 (over z).
Axes of the slice: x: 4, y: 4, z: 4, core: 2. Of those that a mesh axis runs over, the one named last changes fastest.
Arguments:
- tokens: bfloat16 [8192, 3072], P('ctx', 'head'), may hold values from -6 to 6
- w_qkv: bfloat16 [3, 3072, 3072], P(None, None, 'head'), may hold values from -0.109375 to 0.109375
- w_out: bfloat16 [3072, 3072], P('head'), may hold values from -2 to 2
- block_perm: int32 [128], replicated, may hold values from 0 to 127, as said below
Outputs:
- mixed: bfloat16 [8192, 3072], P('ctx', 'head')
The draws below stay inside these ranges and needn't reach their ends.
Inputs may be any that keep to these rules, and one draw needn't show every extreme that they name: A permutation; slot s holds frame row block_perm[s], token rows s * 64 to (s + 1) * 64 - 1 of tokens. Cut the frame rows into 64 runs of 2 consecutive rows, numbered 0 up; each index of ctx holds, for one c of its own, run c in its first 2 slots and run 2 * 32 - 1 - c in its last 2 slots, in row order.
All inputs are finite; a program needn't handle non-finite values.
Results may differ from the reference program's by a relative error of at most 0.02.
Values may be sent and summed in bfloat16 or wider, within the bound.
A program may use at most 192 MiB of HBM per device.

```python
import jax
import jax.numpy as jnp
from jax import lax

D = 3072
HEADS = 24
HD = 128
WW = 64
F = 8
BPD = 4
NB = 128
TOKENS = 8192


def draw_block_perm(key, part):
    holders = NB // BPD
    run_len = BPD // 2
    order = jax.random.permutation(key, holders).astype(jnp.int32)
    slot_ids = jnp.arange(NB, dtype=jnp.int32)
    holder = slot_ids // BPD
    inside = slot_ids % BPD
    run_id = order[holder]
    early = run_id * run_len + inside
    late = (2 * holders - 1 - run_id) * run_len + inside - run_len
    return jnp.where(inside < run_len, early, late).astype(jnp.int32)


def levels(rng, shape, shards, smallest, top_value):
    def one(axis_at, shards_of):
        draws = jax.random.uniform(jax.random.fold_in(jax.random.fold_in(rng, 6), axis_at), (shards_of,), jnp.float32, smallest / len(shards), top_value / len(shards))
        return jnp.repeat(jnp.exp(draws), shape[axis_at] // shards_of).reshape((-1,) + (1,) * (len(shape) - axis_at - 1))

    factor_of = one(*shards[0])
    for cut in shards[1:]:
        factor_of = factor_of * one(*cut)
    return factor_of


def bell_draw(stream_key, dims, scale, limit, cuts=(), held_as=jnp.bfloat16):
    values = jax.random.normal(stream_key, dims, jnp.float32) * scale
    if len(cuts) > 0:
        values = levels(stream_key, dims, cuts, -0.22, 0.18) * values
    return jnp.clip(values, min=-limit, max=limit).astype(held_as)


def setup_inputs(seed: int = 0) -> dict:
    keys = jax.random.split(jax.random.key(seed), 5)
    return {
        "tokens": bell_draw(keys[0], (TOKENS, D), 1.0, 6.0, ((0, 32), (1, 4))),
        "w_qkv": bell_draw(keys[1], (3, D, D), D ** -0.5, 0.109375, ((2, 4),)),
        "w_out": bell_draw(keys[2], (D, D), (HD // 16) ** -0.5, 2.0, ((0, 4),)),
        "block_perm": draw_block_perm(jax.random.fold_in(keys[4], 71), 0),
    }


ROPE_BASE = 10000.0
EPSILON = 1e-06

def frames_and_rows(block_perm, frame_total):
    frame_rows = block_perm.shape[0] // frame_total
    slot_frame = (block_perm // frame_rows).astype(jnp.int32)
    slot_row = (block_perm % frame_rows).astype(jnp.int32)
    return (slot_frame, slot_row)

def rope_angles(frame_of_block, row_of_block, block_width, head_size):
    grid_shape = (frame_of_block.shape[0], block_width)
    pos_frame = jnp.broadcast_to(frame_of_block[:, None], grid_shape).reshape(-1).astype(jnp.float32)
    pos_row = jnp.broadcast_to(row_of_block[:, None], grid_shape).reshape(-1).astype(jnp.float32)
    pos_column = jnp.broadcast_to(jnp.arange(block_width, dtype=jnp.int32)[None, :], grid_shape).reshape(-1).astype(jnp.float32)
    pair_counts = (head_size // 16, 7 * head_size // 32, 7 * head_size // 32)
    angle_parts = []
    for position, pair_count in zip((pos_frame, pos_row, pos_column), pair_counts):
        frequency = ROPE_BASE ** (-jnp.arange(pair_count, dtype=jnp.float32) / pair_count)
        angle_parts.append(position[:, None] * frequency[None, :])
    return angle_parts

def normalize(vector):
    return vector * lax.rsqrt(lax.optimization_barrier(jnp.mean(vector * vector, axis=-1, keepdims=True)) + EPSILON)

def rotate(vector, angle_parts):
    pieces = []
    offset = 0
    for angle_part in angle_parts:
        pair_count = angle_part.shape[1]
        lower_half = vector[..., offset:offset + pair_count]
        upper_half = vector[..., offset + pair_count:offset + 2 * pair_count]
        cosine = jnp.cos(angle_part)[:, None, :]
        sine_part = jnp.sin(angle_part)[:, None, :]
        pieces.append(lower_half * cosine - upper_half * sine_part)
        pieces.append(lower_half * sine_part + upper_half * cosine)
        offset = offset + 2 * pair_count
    return jnp.concatenate(pieces, axis=-1)

def reference(tokens, w_qkv, w_out, block_perm):
    tok_total = tokens.shape[0]
    slot_frame, slot_row = frames_and_rows(block_perm, F)
    angle_parts = rope_angles(slot_frame, slot_row, WW, HD)
    query_raw = jnp.dot(tokens, w_qkv[0], preferred_element_type=jnp.float32).reshape(tok_total, HEADS, HD)
    key_raw = jnp.dot(tokens, w_qkv[1], preferred_element_type=jnp.float32).reshape(tok_total, HEADS, HD)
    value_data = jnp.dot(tokens, w_qkv[2], preferred_element_type=jnp.float32).astype(jnp.bfloat16).reshape(tok_total, HEADS, HD)
    q_rot = rotate(normalize(query_raw), angle_parts).astype(jnp.bfloat16)
    k_rot = rotate(normalize(key_raw), angle_parts).astype(jnp.bfloat16)
    block_ok = (slot_frame[None, :] <= slot_frame[:, None]).astype(jnp.float32)
    slots = slot_frame.shape[0]
    token_ok = jnp.broadcast_to(block_ok[:, None, :, None], (slots, WW, slots, WW)).reshape(tok_total, tok_total)

    def one_head(head_id):
        query_head = lax.dynamic_index_in_dim(q_rot, head_id, 1, keepdims=False)
        key_head = lax.dynamic_index_in_dim(k_rot, head_id, 1, keepdims=False)
        value_head = lax.dynamic_index_in_dim(value_data, head_id, 1, keepdims=False)
        scores = jnp.dot(query_head, key_head.T, preferred_element_type=jnp.float32) * HD ** (-0.5)
        weights = jnp.exp(scores) * token_ok
        denominator = lax.optimization_barrier(jnp.sum(weights, axis=1))
        numerator = jnp.dot(weights.astype(jnp.bfloat16), value_head, preferred_element_type=jnp.float32)
        return (numerator / denominator[:, None]).astype(jnp.bfloat16)
    per_head = lax.map(one_head, jnp.arange(HEADS, dtype=jnp.int32))
    attention = jnp.transpose(per_head, (1, 0, 2)).reshape(tok_total, HEADS * HD)
    return jnp.dot(attention, w_out, preferred_element_type=jnp.float32).astype(jnp.bfloat16)
```

```python
import functools
import math

import jax
import jax.numpy as jnp
import numpy as np
from jax import lax
from jax.experimental import pallas as pl
from jax.experimental.pallas import tpu as pltpu
from jax.sharding import PartitionSpec as P

HD = 128
WW = 64
ROPE_BASE = 10000.0
EPSILON = 1e-06
N = 4
R = 128
HH = 3
HW = HH * HD
DW = 2 * HW
OB = R + 8
BF = jnp.bfloat16
F32 = jnp.float32
RIGHT, LEFT = 0, 1
STEP = (1, N - 1)


def rope_tables(frame_rows):
    parts = ((0, HD // 16), (HD // 8, 7 * HD // 32), (HD // 8 + 7 * HD // 16, 7 * HD // 32))
    frames = np.arange(128) // frame_rows
    rows = np.arange(128) % frame_rows
    tables = []
    for position, kinds in ((np.stack([frames, rows]), (0, 1)), (np.arange(WW)[None], (2,))):
        cosine = np.zeros((position.shape[1], HD), np.float32)
        sine = np.zeros((position.shape[1], HD), np.float32)
        for at, kind in enumerate(kinds):
            first, pairs = parts[kind]
            freq = np.float32(ROPE_BASE) ** (-np.arange(pairs, dtype=np.float32) / pairs)
            angle = position[at].astype(np.float32)[:, None] * freq[None, :].astype(np.float32)
            cosine[:, first : first + pairs] = np.cos(angle)
            cosine[:, first + pairs : first + 2 * pairs] = np.cos(angle)
            sine[:, first : first + pairs] = -np.sin(angle)
            sine[:, first + pairs : first + 2 * pairs] = np.sin(angle)
        tables += [cosine, sine]
    return tables


def kernel(
    perm, frc, frs, coc, cos_, tok, wqkv, wout, out,
    xg, wq, wo, acc, cost, sint, okv, oq, kv, qb, num, den,
    os1, or1, os2, or2, oss, ors, attn, zs1, zr1, zp, zs2, zr2,
    lsem, gs, gr, xs, xr, o1s, o1r, o2s, o2r, oqs, oqr, zss, zsr,
):
    ctx = lax.axis_index("ctx")
    z = lax.axis_index("head")
    c = ctx % 2
    x = (ctx // 2) % N
    y = ctx // (2 * N)

    def cid(yy, xx, cc):
        return (yy * N + xx) * 2 + cc

    def kv_to(half, d):
        if half == 0:
            return cid(y, (x + d) % N, 0)
        return cid((y + d) % N, x, 1)

    def q_to(half, d):
        if half == 0:
            return cid((y + d) % N, x, 0)
        return cid(y, (x + d) % N, 1)

    def my_kv(d):
        return cid((y + c * d) % N, (x + (1 - c) * d) % N, c)

    def my_q(d, core):
        return cid((y + (1 - c) * d) % N, (x + c * d) % N, core)

    sibling = cid(y, x, 1 - c)
    kc = x * (1 - c) + y * c
    qc = y * (1 - c) + x * c
    pending = []

    def send(src, dst, ss, rs, to_ctx, to_z):
        copy = pltpu.make_async_remote_copy(
            src_ref=src, dst_ref=dst, send_sem=ss, recv_sem=rs,
            device_id=(to_ctx, to_z), device_id_type=pl.DeviceIdType.MESH,
        )
        copy.start()
        pending.append(copy)

    def arrive(dst, rs):
        pltpu.make_async_remote_copy(
            src_ref=dst, dst_ref=dst, send_sem=rs, recv_sem=rs,
            device_id=(sibling, z), device_id_type=pl.DeviceIdType.MESH,
        ).wait_recv()

    tok_in = [
        pltpu.make_async_copy(tok.at[pl.ds(h * R, R)], xg.at[h, z], lsem.at[h]) for h in range(2)
    ]
    for copy in tok_in:
        copy.start()
    rel_order = (0, 3, 1, 2)
    w_in = []
    for at, rel in enumerate(rel_order):
        rows = pl.ds(pl.multiple_of((z + rel) % N * DW, DW), DW)
        for j in range(3):
            w_in.append(
                pltpu.make_async_copy(wqkv.at[j, rows], wq.at[j, rows], lsem.at[2 + at * 3 + j])
            )
    for copy in w_in:
        copy.start()
    wo_in = pltpu.make_async_copy(wout, wo, lsem.at[14])
    wo_in.start()

    barrier = pltpu.get_barrier_semaphore()
    peers = [(sibling, z)]
    for d in STEP:
        peers.append((ctx, (z + d) % N))
        for core in range(2):
            peers.append((cid(y, (x + d) % N, core), z))
            peers.append((cid((y + d) % N, x, core), z))
    for peer in peers:
        pl.semaphore_signal(barrier, inc=1, device_id=peer, device_id_type=pl.DeviceIdType.MESH)
    pl.semaphore_wait(barrier, len(peers))

    def gather_own(h):
        for way in (RIGHT, LEFT):
            send(xg.at[h, z], xg.at[h, z], gs.at[h, way], gr.at[h, way], ctx, (z + STEP[way]) % N)

    def gather_relay(h):
        left, right = (z + 3) % N, (z + 1) % N
        arrive(xg.at[h, left], gr.at[h, RIGHT])
        lo, hi = pl.ds(0, R // 2), pl.ds(R // 2, R // 2)
        send(xg.at[h, left, lo], xg.at[h, left, lo], gs.at[h, 2], gr.at[h, 2], ctx, right)
        arrive(xg.at[h, right], gr.at[h, LEFT])
        send(xg.at[h, right, hi], xg.at[h, right, hi], gs.at[h, 3], gr.at[h, 3], ctx, left)

    def gather_last(h):
        far = (z + 2) % N
        arrive(xg.at[h, far, pl.ds(0, R // 2)], gr.at[h, 2])
        arrive(xg.at[h, far, pl.ds(R // 2, R // 2)], gr.at[h, 3])

    def weights(at):
        for j in range(3):
            w_in[at * 3 + j].wait()

    def project(hs, rel, first):
        src = (z + rel) % N
        rows = pl.ds(pl.multiple_of(src * DW, DW), DW)

        def tile(t, carry):
            cols = pl.ds(pl.multiple_of(t % 3 * 256, 256), 256)
            at = pl.ds(pl.multiple_of(t * 256, 256), 256)
            w = wq[t // 3, rows, cols]
            if len(hs) == 2:
                a = jnp.concatenate([xg[h, src] for h in hs], axis=0)
            else:
                a = xg[hs[0], src]
            part = jnp.dot(a, w, preferred_element_type=F32)
            for n, h in enumerate(hs):
                piece = part[n * R : (n + 1) * R]
                if first:
                    acc[h, :, at] = piece
                else:
                    acc[h, :, at] += piece
            return carry

        lax.fori_loop(0, 9, tile, 0)

    def tables():
        for s in range(4):
            at = perm[4 * ctx + s]
            rows = pl.ds(s * WW, WW)
            cost[rows, :] = frc[pl.ds(at, 1), :] + coc[...]
            sint[rows, :] = frs[pl.ds(at, 1), :] + cos_[...]

    def finish(h):
        rows = pl.ds(h * R, R)
        lane = lax.broadcasted_iota(jnp.int32, (R, HD), 1)
        wide = lane >= 16
        low = (lane < 8) | ((lane >= 16) & (lane < 44)) | ((lane >= 72) & (lane < 100))

        def turned(v, scale):
            square = jnp.mean(v * v, axis=-1, keepdims=True)
            v = v * (lax.rsqrt(square + EPSILON) * scale)
            up = jnp.where(wide, pltpu.roll(v, HD - 28, 1), pltpu.roll(v, HD - 8, 1))
            down = jnp.where(wide, pltpu.roll(v, 28, 1), pltpu.roll(v, 8, 1))
            return (v * cost[rows, :] + jnp.where(low, up, down) * sint[rows, :]).astype(BF)

        for half in range(2):
            for i in range(HH):
                to = pl.ds(i * HD, HD)
                col = (half * HH + i) * HD
                oq[half, h, :, to] = turned(acc[h, :, pl.ds(col, HD)], HD**-0.5 / math.log(2.0))
                okv[half, h, :, to] = turned(acc[h, :, pl.ds(DW + col, HD)], 1.0)
                okv[half, h, :, pl.ds(HW + i * HD, HD)] = acc[h, :, pl.ds(2 * DW + col, HD)].astype(
                    BF
                )

    def spread(h):
        for half in range(2):
            kslot, qslot = ((x, y), (y, x))[half]
            for way in (RIGHT, LEFT):
                send(
                    oq.at[half, h], qb.at[h, qslot, c], xs.at[1, h, half * 2 + way],
                    xr.at[1, h, 1 + 2 * way + c], q_to(half, STEP[way]), z,
                )
                send(
                    okv.at[half, h], kv.at[h, kslot, c], xs.at[0, h, half * 2 + way],
                    xr.at[0, h, 1 + 2 * way + c], kv_to(half, STEP[way]), z,
                )
        send(okv.at[1 - c, h], kv.at[h, qc, c], xs.at[0, h, 4], xr.at[0, h, 0], sibling, z)
        send(oq.at[1 - c, h], qb.at[h, kc, c], xs.at[1, h, 4], xr.at[1, h, 0], sibling, z)
        kv[h, kc, c] = okv[c, h]
        qb[h, qc, c] = oq[c, h]

    def spread_relay(h):
        for way in (RIGHT, LEFT):
            kslot = (kc + N - STEP[way]) % N
            qslot = (qc + N - STEP[way]) % N
            for core in range(2):
                arrive(qb.at[h, qslot, core], xr.at[1, h, 1 + 2 * way + core])
            send(
                qb.at[h, qslot, way], qb.at[h, qslot, way], xs.at[1, h, 5 + way],
                xr.at[1, h, 5 + way], my_q(STEP[way], c), z,
            )
            for core in range(2):
                arrive(kv.at[h, kslot, core], xr.at[0, h, 1 + 2 * way + core])
            send(
                kv.at[h, kslot, way], kv.at[h, kslot, way], xs.at[0, h, 5 + way],
                xr.at[0, h, 5 + way], my_kv(STEP[way]), z,
            )
        arrive(kv.at[h, kc, 1 - c], xr.at[0, h, 0])
        arrive(qb.at[h, qc, 1 - c], xr.at[1, h, 0])

    def spread_last(h):
        for way in (RIGHT, LEFT):
            arrive(qb.at[h, (qc + 2) % N, way], xr.at[1, h, 5 + way])
            arrive(kv.at[h, (kc + 2) % N, way], xr.at[0, h, 5 + way])

    frame_rows = perm.shape[0] // 8

    def attend(hq, hk, rel, masked, first):
        slot = (qc + rel) % N
        if masked:
            fq = [
                perm[4 * cid((1 - c) * slot + c * y, (1 - c) * x + c * slot, a) + 2 * hq] // frame_rows
                for a in range(2)
            ]
            fk = [
                perm[4 * cid((1 - c) * y + c * t, (1 - c) * t + c * x, b) + 2 * hk] // frame_rows
                for t in range(N)
                for b in range(2)
            ]
            ok = [[(k <= q).astype(F32) for k in fk] for q in fq]

        for i in range(HH):
            cols = pl.ds(i * HD, HD)
            vcols = pl.ds(HW + i * HD, HD)
            q = qb[hq, slot, :, :, cols].reshape(2 * R, HD)
            k = kv[hk, :, :, :, cols].reshape(2 * N * R, HD)
            v = kv[hk, :, :, :, vcols].reshape(2 * N * R, HD)
            s = lax.dot_general(q, k, (((1,), (1,)), ((), ())), preferred_element_type=F32)
            w = jnp.exp2(s)
            if masked:
                w = jnp.concatenate(
                    [
                        jnp.concatenate(
                            [
                                w[a * R : (a + 1) * R, b * R : (b + 1) * R] * ok[a][b]
                                for b in range(2 * N)
                            ],
                            axis=1,
                        )
                        for a in range(2)
                    ],
                    axis=0,
                )
            total = w[:, :HD]
            for b in range(1, 2 * N):
                total = total + w[:, b * HD : (b + 1) * HD]
            o = jnp.dot(w.astype(BF), v, preferred_element_type=F32)
            for a in range(2):
                rows = slice(a * R, (a + 1) * R)
                if first:
                    num[hq, slot, a, :, cols] = o[rows]
                    den[hq, slot, a, :, cols] = total[rows]
                else:
                    num[hq, slot, a, :, cols] += o[rows]
                    den[hq, slot, a, :, cols] += total[rows]

    def row_sum(h, slot, core, i):
        return jnp.sum(den[h, slot, core, :, pl.ds(i * HD, HD)].T, axis=0, keepdims=True)

    def pack(dst, h, slot, core, plus=None):
        for i in range(HH):
            cols = pl.ds(i * HD, HD)
            n = num[h, slot, core, :, cols]
            d = row_sum(h, slot, core, i)
            if plus is not None:
                n = n + plus[pl.ds(0, R), cols].astype(F32)
                d = d + plus[pl.ds(R, 8), cols].astype(F32)
            dst[pl.ds(0, R), cols] = n.astype(BF)
            dst[pl.ds(R, 8), cols] = jnp.broadcast_to(d, (8, HD)).astype(BF)

    def sum_far(h):
        far = (qc + 2) % N
        for way in (RIGHT, LEFT):
            pack(os1.at[h, way], h, far, way)
            send(
                os1.at[h, way], or1.at[h, way], o1s.at[h, way], o1r.at[h, way],
                my_q(STEP[way], c), z,
            )

    def sum_near(h):
        for way in (RIGHT, LEFT):
            slot = (qc + STEP[way]) % N
            arrive(or1.at[h, way], o1r.at[h, way])
            for core in range(2):
                pack(os2.at[h, way, core], h, slot, core, or1.at[h, way] if core == way else None)
                send(
                    os2.at[h, way, core], or2.at[h, c, way], o2s.at[h, way, core],
                    o2r.at[h, c, way], my_q(STEP[way], core), z,
                )

    def sum_sibling(h):
        pack(oss.at[h], h, qc, 1 - c)
        send(oss.at[h], ors.at[h], oqs.at[h], oqr.at[h], sibling, z)

    def normalize(h):
        for half in range(2):
            for way in (RIGHT, LEFT):
                arrive(or2.at[h, half, way], o2r.at[h, half, way])
        arrive(ors.at[h], oqr.at[h])
        for mine in range(2):
            half = c if mine else 1 - c
            for i in range(HH):
                cols = pl.ds(i * HD, HD)
                if mine:
                    n = num[h, qc, c, :, cols]
                    d = row_sum(h, qc, c, i)
                else:
                    n = ors[h, pl.ds(0, R), cols].astype(F32)
                    d = ors[h, pl.ds(R, 8), cols].astype(F32)[:1]
                for way in (RIGHT, LEFT):
                    n = n + or2[h, half, way, pl.ds(0, R), cols].astype(F32)
                    d = d + or2[h, half, way, pl.ds(R, 8), cols].astype(F32)[:1]
                attn[h, half, :, cols] = (n / jnp.broadcast_to(d, (HD, R)).T).astype(BF)

    def mixed_for(h, rel, store):
        base = (z + rel) % N * DW

        for t in range(3):
            cols = pl.ds(pl.multiple_of(base + t * 256, 256), 256)
            part = jnp.dot(attn[h, 0], wo[pl.ds(0, HW), cols], preferred_element_type=F32)
            part += jnp.dot(attn[h, 1], wo[pl.ds(HW, HW), cols], preferred_element_type=F32)
            store(pl.ds(t * 256, 256), part)

    def mix_far(h):
        def store(cols, part):
            zs1[h, RIGHT, :, cols] = part[: R // 2].astype(BF)
            zs1[h, LEFT, :, cols] = part[R // 2 :].astype(BF)

        mixed_for(h, 2, store)
        for way in (RIGHT, LEFT):
            send(
                zs1.at[h, way], zr1.at[h, way], zss.at[h, 0, way], zsr.at[h, 0, way],
                ctx, (z + STEP[way]) % N,
            )

    def mix_rest(h):
        for at, rel in enumerate((1, 3, 0)):

            def store(cols, part, at=at):
                zp[h, at, :, cols] = part

            mixed_for(h, rel, store)

    def mix_near(h):
        lo, hi = pl.ds(0, R // 2), pl.ds(R // 2, R // 2)
        for way in (RIGHT, LEFT):
            summed, plain = ((lo, hi), (hi, lo))[way]
            zs2[h, way, plain] = zp[h, way, plain].astype(BF)
            arrive(zr1.at[h, way], zsr.at[h, 0, way])
            zs2[h, way, summed] = (zp[h, way, summed] + zr1[h, way].astype(F32)).astype(BF)
            send(
                zs2.at[h, way], zr2.at[h, way], zss.at[h, 1, way], zsr.at[h, 1, way],
                ctx, (z + STEP[way]) % N,
            )

    def mix_last(h):
        total = zp[h, 2]
        for way in (RIGHT, LEFT):
            arrive(zr2.at[h, way], zsr.at[h, 1, way])
            total = total + zr2[h, way].astype(F32)
        out[pl.ds(h * R, R), :] = total.astype(BF)

    tok_in[0].wait()
    gather_own(0)
    tok_in[1].wait()
    tables()
    weights(0)
    project((0, 1), 0, True)
    gather_relay(0)
    gather_own(1)
    weights(1)
    project((0,), 3, False)
    weights(2)
    project((0,), 1, False)
    weights(3)
    gather_last(0)
    project((0,), 2, False)
    finish(0)
    spread(0)
    gather_relay(1)
    project((1,), 3, False)
    project((1,), 1, False)
    gather_last(1)
    project((1,), 2, False)
    finish(1)
    spread_relay(0)
    spread(1)
    spread_last(0)
    attend(0, 0, 2, True, True)
    sum_far(0)
    for rel in (1, 3, 0):
        attend(0, 0, rel, True, True)
    spread_relay(1)
    sum_near(0)
    sum_sibling(0)
    for rel in (1, 3, 0):
        attend(1, 0, rel, False, True)
    wo_in.wait()
    normalize(0)
    mix_far(0)
    mix_rest(0)
    spread_last(1)
    attend(1, 0, 2, False, True)
    attend(1, 1, 2, True, False)
    sum_far(1)
    mix_near(0)
    for rel in (1, 3):
        attend(1, 1, rel, True, False)
    sum_near(1)
    attend(1, 1, 0, True, False)
    sum_sibling(1)
    mix_last(0)
    normalize(1)
    mix_far(1)
    mix_rest(1)
    mix_near(1)
    mix_last(1)
    for copy in pending:
        copy.wait_send()


def per_device(tokens, w_qkv, w_out, block_perm):
    frc, frs, coc, cos_ = [jnp.asarray(t) for t in rope_tables(block_perm.shape[0] // 8)]
    vmem = pl.BlockSpec(memory_space=pltpu.VMEM)
    hbm = pl.BlockSpec(memory_space=pl.ANY)
    dma = pltpu.SemaphoreType.DMA
    return pl.pallas_call(
        kernel,
        name="attention_layer",
        out_shape=jax.ShapeDtypeStruct((2 * R, DW), BF),
        in_specs=[pl.BlockSpec(memory_space=pltpu.SMEM)] + [vmem] * 4 + [hbm] * 3,
        out_specs=vmem,
        scratch_shapes=[
            pltpu.VMEM((2, N, R, DW), BF),
            pltpu.VMEM((3, N * DW, DW), BF),
            pltpu.VMEM((DW, N * DW), BF),
            pltpu.VMEM((2, R, 3 * DW), F32),
            pltpu.VMEM((2 * R, HD), F32),
            pltpu.VMEM((2 * R, HD), F32),
            pltpu.VMEM((2, 2, R, DW), BF),
            pltpu.VMEM((2, 2, R, HW), BF),
            pltpu.VMEM((2, N, 2, R, DW), BF),
            pltpu.VMEM((2, N, 2, R, HW), BF),
            pltpu.VMEM((2, N, 2, R, HW), F32),
            pltpu.VMEM((2, N, 2, R, HW), F32),
            pltpu.VMEM((2, 2, OB, HW), BF),
            pltpu.VMEM((2, 2, OB, HW), BF),
            pltpu.VMEM((2, 2, 2, OB, HW), BF),
            pltpu.VMEM((2, 2, 2, OB, HW), BF),
            pltpu.VMEM((2, OB, HW), BF),
            pltpu.VMEM((2, OB, HW), BF),
            pltpu.VMEM((2, 2, R, HW), BF),
            pltpu.VMEM((2, 2, R // 2, DW), BF),
            pltpu.VMEM((2, 2, R // 2, DW), BF),
            pltpu.VMEM((2, 3, R, DW), F32),
            pltpu.VMEM((2, 2, R, DW), BF),
            pltpu.VMEM((2, 2, R, DW), BF),
            dma((15,)),
            dma((2, 4)),
            dma((2, 4)),
            dma((2, 2, 7)),
            dma((2, 2, 7)),
            dma((2, 2)),
            dma((2, 2)),
            dma((2, 2, 2)),
            dma((2, 2, 2)),
            dma((2,)),
            dma((2,)),
            dma((2, 2, 2)),
            dma((2, 2, 2)),
        ],
        compiler_params=pltpu.CompilerParams(
            collective_id=0, has_side_effects=True, vmem_limit_bytes=64 * 1024 * 1024 - 65536
        ),
    )(block_perm, frc, frs, coc, cos_, tokens, w_qkv, w_out)


def solution(mesh):
    in_specs = (P("ctx", "head"), P(None, None, "head"), P("head", None), P())
    return jax.shard_map(
        per_device, mesh=mesh, in_specs=in_specs, out_specs=P("ctx", "head"), check_vma=False
    )
```

```python
import functools
import math

import jax
import jax.numpy as jnp
import numpy as np
from jax import lax
from jax.experimental import pallas as pl
from jax.experimental.pallas import tpu as pltpu
from jax.sharding import PartitionSpec as P

HD = 128
WW = 64
ROPE_BASE = 10000.0
EPSILON = 1e-06
N = 4
R = 128
HH = 3
HW = HH * HD
DW = 2 * HW
OB = R + 8
BF = jnp.bfloat16
F32 = jnp.float32
RIGHT, LEFT = 0, 1
STEP = (1, N - 1)


def rope_tables(frame_rows):
    parts = ((0, HD // 16), (HD // 8, 7 * HD // 32), (HD // 8 + 7 * HD // 16, 7 * HD // 32))
    frames = np.arange(128) // frame_rows
    rows = np.arange(128) % frame_rows
    tables = []
    for position, kinds in ((np.stack([frames, rows]), (0, 1)), (np.arange(WW)[None], (2,))):
        cosine = np.zeros((position.shape[1], HD), np.float32)
        sine = np.zeros((position.shape[1], HD), np.float32)
        for at, kind in enumerate(kinds):
            first, pairs = parts[kind]
            freq = np.float32(ROPE_BASE) ** (-np.arange(pairs, dtype=np.float32) / pairs)
            angle = position[at].astype(np.float32)[:, None] * freq[None, :].astype(np.float32)
            cosine[:, first : first + pairs] = np.cos(angle)
            cosine[:, first + pairs : first + 2 * pairs] = np.cos(angle)
            sine[:, first : first + pairs] = -np.sin(angle)
            sine[:, first + pairs : first + 2 * pairs] = np.sin(angle)
        tables += [cosine, sine]
    return tables


def kernel(
    perm_hbm, tab_hbm, tok, wqkv, wout, out,
    perm, tab, xg, wq, wo, acc, cost, sint, swap, okv, oq, kv, qb, num, den,
    os1, or1, os2, or2, oss, ors, attn, zs1, zr1, zp, own, zs2, zr2, mixed,
    lsem, gs, gr, ks, kr, krs, krr, qs, qr, qrs, qrr, sbs, sbr,
    o1s, o1r, o2s, o2r, oqs, oqr, z1s, z1r, z2s, z2r,
):
    ctx = lax.axis_index("ctx")
    z = lax.axis_index("head")
    c = ctx % 2
    x = (ctx // 2) % N
    y = ctx // (2 * N)

    def cid(yy, xx, cc):
        return (yy * N + xx) * 2 + cc

    def kv_to(half, d):
        if half == 0:
            return cid(y, (x + d) % N, 0)
        return cid((y + d) % N, x, 1)

    def q_to(half, d):
        if half == 0:
            return cid((y + d) % N, x, 0)
        return cid(y, (x + d) % N, 1)

    def my_kv(d):
        return cid((y + c * d) % N, (x + (1 - c) * d) % N, c)

    def my_q(d, core):
        return cid((y + (1 - c) * d) % N, (x + c * d) % N, core)

    sibling = cid(y, x, 1 - c)
    kc = x * (1 - c) + y * c
    qc = y * (1 - c) + x * c
    pending = []

    def send(src, dst, ss, rs, to_ctx, to_z):
        copy = pltpu.make_async_remote_copy(
            src_ref=src, dst_ref=dst, send_sem=ss, recv_sem=rs,
            device_id=(to_ctx, to_z), device_id_type=pl.DeviceIdType.MESH,
        )
        copy.start()
        pending.append(copy)

    def arrive(dst, rs):
        pltpu.make_async_remote_copy(
            src_ref=dst, dst_ref=dst, send_sem=rs, recv_sem=rs,
            device_id=(sibling, z), device_id_type=pl.DeviceIdType.MESH,
        ).wait_recv()

    perm_in = pltpu.make_async_copy(perm_hbm, perm, lsem.at[15])
    perm_in.start()
    tab_in = pltpu.make_async_copy(tab_hbm, tab, lsem.at[16])
    tab_in.start()
    tok_in = [
        pltpu.make_async_copy(tok.at[pl.ds(h * R, R)], xg.at[h, z], lsem.at[h]) for h in range(2)
    ]
    for copy in tok_in:
        copy.start()
    rel_order = (0, 3, 1, 2)
    w_in = []
    for at, rel in enumerate(rel_order):
        rows = pl.ds(pl.multiple_of((z + rel) % N * DW, DW), DW)
        for j in range(3):
            w_in.append(
                pltpu.make_async_copy(wqkv.at[j, rows], wq.at[j, rows], lsem.at[2 + at * 3 + j])
            )
    for copy in w_in:
        copy.start()
    wo_in = pltpu.make_async_copy(wout, wo, lsem.at[14])
    wo_in.start()

    barrier = pltpu.get_barrier_semaphore()
    peers = [(sibling, z)]
    for d in STEP:
        peers.append((ctx, (z + d) % N))
        for core in range(2):
            peers.append((cid(y, (x + d) % N, core), z))
            peers.append((cid((y + d) % N, x, core), z))
    for peer in peers:
        pl.semaphore_signal(barrier, inc=1, device_id=peer, device_id_type=pl.DeviceIdType.MESH)
    pl.semaphore_wait(barrier, len(peers))

    half_rows = (pl.ds(0, R // 2), pl.ds(R // 2, R // 2))

    def gather_own(h):
        for turn in range(2):
            for way in (RIGHT, LEFT):
                part = way ^ turn
                block = xg.at[h, z, half_rows[part]]
                to = (z + STEP[way]) % N
                send(block, block, gs.at[h, way, part], gr.at[h, way, part], ctx, to)

    def gather_relay(h):
        for way in (RIGHT, LEFT):
            block = xg.at[h, (z + N - STEP[way]) % N, half_rows[way]]
            arrive(block, gr.at[h, way, way])
            send(block, block, gs.at[h, 2, way], gr.at[h, 2, way], ctx, (z + STEP[way]) % N)

    def gather_rest(h, way):
        part = 1 - way
        arrive(xg.at[h, (z + N - STEP[way]) % N, half_rows[part]], gr.at[h, way, part])

    def gather_last(h):
        for way in (RIGHT, LEFT):
            arrive(xg.at[h, (z + 2) % N, half_rows[way]], gr.at[h, 2, way])

    def weights(at):
        for j in range(3):
            w_in[at * 3 + j].wait()

    def project(hs, rel, first):
        src = (z + rel) % N
        rows = pl.ds(pl.multiple_of(src * DW, DW), DW)

        def tile(j, carry):
            at = pl.ds(pl.multiple_of(j * DW, DW), DW)
            w = wq[j, rows, :]
            if len(hs) == 2:
                a = jnp.concatenate([xg[h, src] for h in hs], axis=0)
            else:
                a = xg[hs[0], src]
            part = jnp.dot(a, w, preferred_element_type=F32)
            for n, h in enumerate(hs):
                piece = part[n * R : (n + 1) * R]
                if first:
                    acc[h, :, at] = piece
                else:
                    acc[h, :, at] += piece
            return carry

        lax.fori_loop(0, 3, tile, 0)

    def tables():
        perm_in.wait()
        tab_in.wait()
        for s in range(4):
            at = perm[4 * ctx + s]
            rows = pl.ds(s * WW, WW)
            cost[rows, :] = tab[pl.ds(at, 1), :] + tab[pl.ds(256, WW), :]
            sint[rows, :] = tab[pl.ds(128 + at, 1), :] + tab[pl.ds(256 + WW, WW), :]
        source = lax.broadcasted_iota(jnp.int32, (2 * HD, 2 * HD), 0)
        target = lax.broadcasted_iota(jnp.int32, (2 * HD, 2 * HD), 1)
        lane = target % HD
        distance = jnp.where(lane < 16, 8, 28)
        low = (lane < 8) | ((lane >= 16) & (lane < 44)) | ((lane >= 72) & (lane < 100))
        partner = target + jnp.where(low, distance, -distance)
        swap[...] = jnp.where(source == partner, 1.0, 0.0).astype(BF)

    def finish(h):
        rows = pl.ds(h * R, R)
        cosine, sine = cost[rows, :], sint[rows, :]
        for j in range(2):
            pairs = [acc[h, :, pl.ds(j * DW + i * 2 * HD, 2 * HD)] for i in range(HH)]
            stacked = jnp.concatenate([p.astype(BF) for p in pairs], axis=0)
            other = jnp.dot(stacked, swap[...], preferred_element_type=F32)
            for head in range(2 * HH):
                cols = slice(head % 2 * HD, (head % 2 + 1) * HD)
                v = pairs[head // 2][:, cols]
                w = other[head // 2 * R : (head // 2 + 1) * R, cols]
                square = jnp.mean(v * v, axis=-1, keepdims=True)
                factor = lax.rsqrt(square + EPSILON)
                if j == 0:
                    factor = factor * (HD**-0.5 / math.log(2.0))
                turned = ((v * cosine + w * sine) * factor).astype(BF)
                half, to = head // HH, pl.ds(head % HH * HD, HD)
                if j == 0:
                    oq[half, h, :, to] = turned
                else:
                    okv[half, h, 0, :, to] = turned
        for half in range(2):
            okv[half, h, 1] = acc[h, :, pl.ds(2 * DW + half * HW, HW)].astype(BF)

    def spread(h):
        for turn in range(2):
            for half in range(2):
                kslot, qslot = ((x, y), (y, x))[half]
                for way in (RIGHT, LEFT):
                    part = way ^ turn
                    rows = half_rows[part]
                    send(
                        oq.at[half, h, rows], qb.at[h, qslot, c, rows], qs.at[h, half, way, part],
                        qr.at[h, way, part, c], q_to(half, STEP[way]), z,
                    )
                    send(
                        okv.at[half, h, part], kv.at[h, kslot, c, part], ks.at[h, half, way, part],
                        kr.at[h, way, part, c], kv_to(half, STEP[way]), z,
                    )
        send(oq.at[1 - c, h], qb.at[h, kc, c], sbs.at[h, 0], sbr.at[h, 0], sibling, z)
        send(okv.at[1 - c, h], kv.at[h, qc, c], sbs.at[h, 1], sbr.at[h, 1], sibling, z)
        kv[h, kc, c] = okv[c, h]
        qb[h, qc, c] = oq[c, h]

    def spread_relay(h):
        for way in (RIGHT, LEFT):
            kslot = (kc + N - STEP[way]) % N
            qslot = (qc + N - STEP[way]) % N
            for core in range(2):
                block = qb.at[h, qslot, core, half_rows[way]]
                arrive(block, qr.at[h, way, way, core])
                send(block, block, qrs.at[h, way, core], qrr.at[h, way, core], my_q(STEP[way], c), z)
        for way in (RIGHT, LEFT):
            kslot = (kc + N - STEP[way]) % N
            for core in range(2):
                block = kv.at[h, kslot, core, way]
                arrive(block, kr.at[h, way, way, core])
                send(
                    block, block, krs.at[h, way, core], krr.at[h, way, core], my_kv(STEP[way]), z
                )

    def spread_rest(h):
        arrive(qb.at[h, qc, 1 - c], sbr.at[h, 0])
        arrive(kv.at[h, kc, 1 - c], sbr.at[h, 1])
        for way in (RIGHT, LEFT):
            kslot = (kc + N - STEP[way]) % N
            qslot = (qc + N - STEP[way]) % N
            part = 1 - way
            for core in range(2):
                arrive(qb.at[h, qslot, core, half_rows[part]], qr.at[h, way, part, core])
                arrive(kv.at[h, kslot, core, part], kr.at[h, way, part, core])

    def spread_last_q(h):
        for way in (RIGHT, LEFT):
            for core in range(2):
                arrive(qb.at[h, (qc + 2) % N, core, half_rows[way]], qrr.at[h, way, core])

    def spread_last_kv(h):
        for way in (RIGHT, LEFT):
            for core in range(2):
                arrive(kv.at[h, (kc + 2) % N, core, way], krr.at[h, way, core])

    frame_rows = perm.shape[0] // 8

    def attend(hq, hk, rel, krels, masked, first):
        slot = (qc + rel) % N
        kslots = [(kc + krel) % N for krel in krels]
        if masked:
            fq = [
                perm[4 * cid((1 - c) * slot + c * y, (1 - c) * x + c * slot, a) + 2 * hq] // frame_rows
                for a in range(2)
            ]
            fk = [
                perm[4 * cid((1 - c) * y + c * t, (1 - c) * t + c * x, b) + 2 * hk] // frame_rows
                for t in kslots
                for b in range(2)
            ]
            ok = [[(k <= q).astype(F32) for k in fk] for q in fq]

        for i in range(HH):
            cols = pl.ds(i * HD, HD)
            q = qb[hq, slot, :, :, cols].reshape(2 * R, HD)
            k = jnp.concatenate([kv[hk, t, b, 0, :, cols] for t in kslots for b in range(2)], axis=0)
            v = jnp.concatenate([kv[hk, t, b, 1, :, cols] for t in kslots for b in range(2)], axis=0)
            s = lax.dot_general(q, k, (((1,), (1,)), ((), ())), preferred_element_type=F32)
            w = jnp.exp2(s)
            blocks = range(2 * len(krels))
            if masked:
                w = jnp.concatenate(
                    [
                        jnp.concatenate(
                            [w[a * R : (a + 1) * R, b * R : (b + 1) * R] * ok[a][b] for b in blocks],
                            axis=1,
                        )
                        for a in range(2)
                    ],
                    axis=0,
                )
            total = w[:, :HD]
            for b in blocks[1:]:
                total = total + w[:, b * HD : (b + 1) * HD]
            o = jnp.dot(w.astype(BF), v, preferred_element_type=F32)
            for a in range(2):
                rows = slice(a * R, (a + 1) * R)
                if first:
                    num[hq, slot, a, :, cols] = o[rows]
                    den[hq, slot, a, :, cols] = total[rows]
                else:
                    num[hq, slot, a, :, cols] += o[rows]
                    den[hq, slot, a, :, cols] += total[rows]

    def row_sum(h, slot, core, i):
        return jnp.sum(den[h, slot, core, :, pl.ds(i * HD, HD)].T, axis=0, keepdims=True)

    def pack(dst, h, slot, core, plus=None):
        for i in range(HH):
            cols = pl.ds(i * HD, HD)
            n = num[h, slot, core, :, cols]
            d = row_sum(h, slot, core, i)
            if plus is not None:
                n = n + plus[pl.ds(0, R), cols].astype(F32)
                d = d + plus[pl.ds(R, 8), cols].astype(F32)
            dst[pl.ds(0, R), cols] = n.astype(BF)
            dst[pl.ds(R, 8), cols] = jnp.broadcast_to(d, (8, HD)).astype(BF)

    def sum_far(h):
        far = (qc + 2) % N
        for way in (RIGHT, LEFT):
            pack(os1.at[h, way], h, far, way)
            send(
                os1.at[h, way], or1.at[h, way], o1s.at[h, way], o1r.at[h, way],
                my_q(STEP[way], c), z,
            )

    def sum_near(h, way, core, plus=None):
        pack(os2.at[h, way, core], h, (qc + STEP[way]) % N, core, plus)
        send(
            os2.at[h, way, core], or2.at[h, c, way], o2s.at[h, way, core],
            o2r.at[h, c, way], my_q(STEP[way], core), z,
        )

    def sum_plain(h, way):
        sum_near(h, way, 1 - way)

    def sum_passed(h):
        for way in (RIGHT, LEFT):
            arrive(or1.at[h, way], o1r.at[h, way])
            sum_near(h, way, way, or1.at[h, way])

    def sum_sibling(h):
        pack(oss.at[h], h, qc, 1 - c)
        send(oss.at[h], ors.at[h], oqs.at[h], oqr.at[h], sibling, z)

    def normalize(h):
        for half in range(2):
            for way in (RIGHT, LEFT):
                arrive(or2.at[h, half, way], o2r.at[h, half, way])
        arrive(ors.at[h], oqr.at[h])
        for mine in range(2):
            half = c if mine else 1 - c
            for i in range(HH):
                cols = pl.ds(i * HD, HD)
                if mine:
                    n = num[h, qc, c, :, cols]
                    d = row_sum(h, qc, c, i)
                else:
                    n = ors[h, pl.ds(0, R), cols].astype(F32)
                    d = ors[h, pl.ds(R, 8), cols].astype(F32)[:1]
                for way in (RIGHT, LEFT):
                    n = n + or2[h, half, way, pl.ds(0, R), cols].astype(F32)
                    d = d + or2[h, half, way, pl.ds(R, 8), cols].astype(F32)[:1]
                attn[h, half, :, cols] = (n / jnp.broadcast_to(d, (HD, R)).T).astype(BF)

    def mixed_for(h, rel, store):
        base = (z + rel) % N * DW

        for t in range(3):
            cols = pl.ds(pl.multiple_of(base + t * 256, 256), 256)
            part = jnp.dot(attn[h, 0], wo[pl.ds(0, HW), cols], preferred_element_type=F32)
            part += jnp.dot(attn[h, 1], wo[pl.ds(HW, HW), cols], preferred_element_type=F32)
            store(pl.ds(t * 256, 256), part)

    def mix_far(h):
        def store(cols, part):
            for way in (RIGHT, LEFT):
                zs1[h, way, :, cols] = part[way * (R // 2) : (way + 1) * (R // 2)].astype(BF)

        mixed_for(h, 2, store)
        for way in (RIGHT, LEFT):
            send(
                zs1.at[h, way], zr1.at[h, way], z1s.at[h, way], z1r.at[h, way],
                ctx, (z + STEP[way]) % N,
            )

    def mix_send(h, way, part):
        send(
            zs2.at[h, way, part], zr2.at[h, way, part], z2s.at[h, way, part], z2r.at[h, way, part],
            ctx, (z + STEP[way]) % N,
        )

    def mix_plain(h, way):
        part = 1 - way

        def store(cols, rows):
            zp[h, way, :, cols] = rows[way * (R // 2) : (way + 1) * (R // 2)]
            zs2[h, way, part, :, cols] = rows[part * (R // 2) : (part + 1) * (R // 2)].astype(BF)

        mixed_for(h, STEP[way], store)
        mix_send(h, way, part)

    def mix_own(h):
        def store(cols, rows):
            own[h, :, cols] = rows

        mixed_for(h, 0, store)

    def mix_passed(h):
        for way in (RIGHT, LEFT):
            arrive(zr1.at[h, way], z1r.at[h, way])
            zs2[h, way, way] = (zp[h, way] + zr1[h, way].astype(F32)).astype(BF)
            mix_send(h, way, way)

    def mix_last(h):
        for part in (1, 0):
            total = own[h, half_rows[part], :]
            for way in ((RIGHT, LEFT) if part else (LEFT, RIGHT)):
                arrive(zr2.at[h, way, part], z2r.at[h, way, part])
                total = total + zr2[h, way, part].astype(F32)
            mixed[h, half_rows[part], :] = total.astype(BF)
        copy = pltpu.make_async_copy(mixed.at[h], out.at[pl.ds(h * R, R)], lsem.at[h])
        copy.start()
        outgoing.append(copy)

    near = (1, 3, 0)
    every = (1, 3, 0, 2)
    outgoing = []
    tok_in[0].wait()
    gather_own(0)
    tables()
    tok_in[1].wait()
    weights(0)
    project((0, 1), 0, True)
    gather_relay(0)
    gather_own(1)
    weights(1)
    gather_rest(0, RIGHT)
    project((0,), 3, False)
    weights(2)
    gather_rest(0, LEFT)
    project((0,), 1, False)
    weights(3)
    gather_last(0)
    project((0,), 2, False)
    finish(0)
    spread(0)
    gather_relay(1)
    gather_rest(1, RIGHT)
    project((1,), 3, False)
    gather_rest(1, LEFT)
    project((1,), 1, False)
    spread_relay(0)
    gather_last(1)
    project((1,), 2, False)
    finish(1)
    spread(1)
    spread_rest(0)
    spread_last_q(0)
    spread_last_kv(0)
    attend(0, 0, 2, every, True, True)
    attend(0, 0, 1, every, True, True)
    spread_relay(1)
    sum_far(0)
    attend(0, 0, 3, every, True, True)
    attend(0, 0, 0, every, True, True)
    spread_rest(1)
    attend(1, 0, 1, every, False, True)
    sum_plain(0, RIGHT)
    sum_plain(0, LEFT)
    sum_sibling(0)
    attend(1, 0, 3, every, False, True)
    sum_passed(0)
    attend(1, 0, 0, every, False, True)
    attend(1, 1, 1, near, True, False)
    attend(1, 1, 3, near, True, False)
    attend(1, 1, 0, near, True, False)
    spread_last_q(1)
    attend(1, 0, 2, every, False, True)
    spread_last_kv(1)
    attend(1, 1, 2, every, True, False)
    sum_far(1)
    attend(1, 1, 1, (2,), True, False)
    sum_plain(1, RIGHT)
    attend(1, 1, 3, (2,), True, False)
    sum_plain(1, LEFT)
    attend(1, 1, 0, (2,), True, False)
    sum_sibling(1)
    wo_in.wait()
    normalize(0)
    mix_far(0)
    mix_plain(0, RIGHT)
    sum_passed(1)
    mix_plain(0, LEFT)
    mix_own(0)
    mix_passed(0)
    normalize(1)
    mix_far(1)
    mix_plain(1, RIGHT)
    mix_plain(1, LEFT)
    mix_own(1)
    mix_last(0)
    mix_passed(1)
    mix_last(1)
    for copy in outgoing:
        copy.wait()
    for copy in pending:
        copy.wait_send()


def per_device(tokens, w_qkv, w_out, block_perm):
    table = jnp.asarray(np.concatenate(rope_tables(block_perm.shape[0] // 8)))
    hbm = pl.BlockSpec(memory_space=pl.ANY)
    dma = pltpu.SemaphoreType.DMA
    return pl.pallas_call(
        kernel,
        name="attention_layer",
        out_shape=jax.ShapeDtypeStruct((2 * R, DW), BF),
        in_specs=[hbm] * 5,
        out_specs=hbm,
        scratch_shapes=[
            pltpu.SMEM(block_perm.shape, jnp.int32),
            pltpu.VMEM(table.shape, F32),
            pltpu.VMEM((2, N, R, DW), BF),
            pltpu.VMEM((3, N * DW, DW), BF),
            pltpu.VMEM((DW, N * DW), BF),
            pltpu.VMEM((2, R, 3 * DW), F32),
            pltpu.VMEM((2 * R, HD), F32),
            pltpu.VMEM((2 * R, HD), F32),
            pltpu.VMEM((2 * HD, 2 * HD), BF),
            pltpu.VMEM((2, 2, 2, R, HW), BF),
            pltpu.VMEM((2, 2, R, HW), BF),
            pltpu.VMEM((2, N, 2, 2, R, HW), BF),
            pltpu.VMEM((2, N, 2, R, HW), BF),
            pltpu.VMEM((2, N, 2, R, HW), F32),
            pltpu.VMEM((2, N, 2, R, HW), F32),
            pltpu.VMEM((2, 2, OB, HW), BF),
            pltpu.VMEM((2, 2, OB, HW), BF),
            pltpu.VMEM((2, 2, 2, OB, HW), BF),
            pltpu.VMEM((2, 2, 2, OB, HW), BF),
            pltpu.VMEM((2, OB, HW), BF),
            pltpu.VMEM((2, OB, HW), BF),
            pltpu.VMEM((2, 2, R, HW), BF),
            pltpu.VMEM((2, 2, R // 2, DW), BF),
            pltpu.VMEM((2, 2, R // 2, DW), BF),
            pltpu.VMEM((2, 2, R // 2, DW), F32),
            pltpu.VMEM((2, R, DW), F32),
            pltpu.VMEM((2, 2, 2, R // 2, DW), BF),
            pltpu.VMEM((2, 2, 2, R // 2, DW), BF),
            pltpu.VMEM((2, R, DW), BF),
            dma((17,)),
            dma((2, 3, 2)),
            dma((2, 3, 2)),
            dma((2, 2, 2, 2)),
            dma((2, 2, 2, 2)),
            dma((2, 2, 2)),
            dma((2, 2, 2)),
            dma((2, 2, 2, 2)),
            dma((2, 2, 2, 2)),
            dma((2, 2, 2)),
            dma((2, 2, 2)),
            dma((2, 2)),
            dma((2, 2)),
            dma((2, 2)),
            dma((2, 2)),
            dma((2, 2, 2)),
            dma((2, 2, 2)),
            dma((2,)),
            dma((2,)),
            dma((2, 2)),
            dma((2, 2)),
            dma((2, 2, 2)),
            dma((2, 2, 2)),
        ],
        compiler_params=pltpu.CompilerParams(
            collective_id=0, has_side_effects=True, vmem_limit_bytes=64 * 1024 * 1024 - 65536
        ),
    )(block_perm, table, tokens, w_qkv, w_out)


def solution(mesh):
    in_specs = (P("ctx", "head"), P(None, None, "head"), P("head", None), P())
    return jax.shard_map(
        per_device, mesh=mesh, in_specs=in_specs, out_specs=P("ctx", "head"), check_vma=False
    )
```

```python
import functools
import math

import jax
import jax.numpy as jnp
import numpy as np
from jax import lax
from jax.experimental import pallas as pl
from jax.experimental.pallas import tpu as pltpu
from jax.sharding import PartitionSpec as P

HD = 128
WW = 64
ROPE_BASE = 10000.0
EPSILON = 1e-06
N = 4
R = 128
HH = 3
HW = HH * HD
DW = 2 * HW
OB = R + 8
BF = jnp.bfloat16
F32 = jnp.float32
RIGHT, LEFT = 0, 1
EARLY, LATE = 0, 1
C0, C1, C2 = (EARLY, 0, R // 2, 0), (EARLY, R // 2, R // 2, 1), (LATE, 0, R, 2)
STEP = (1, N - 1)


def rope_tables(frame_rows):
    parts = ((0, HD // 16), (HD // 8, 7 * HD // 32), (HD // 8 + 7 * HD // 16, 7 * HD // 32))
    frames = np.arange(128) // frame_rows
    rows = np.arange(128) % frame_rows
    tables = []
    for position, kinds in ((np.stack([frames, rows]), (0, 1)), (np.arange(WW)[None], (2,))):
        cosine = np.zeros((position.shape[1], HD), np.float32)
        sine = np.zeros((position.shape[1], HD), np.float32)
        for at, kind in enumerate(kinds):
            first, pairs = parts[kind]
            freq = np.float32(ROPE_BASE) ** (-np.arange(pairs, dtype=np.float32) / pairs)
            angle = position[at].astype(np.float32)[:, None] * freq[None, :].astype(np.float32)
            cosine[:, first : first + pairs] = np.cos(angle)
            cosine[:, first + pairs : first + 2 * pairs] = np.cos(angle)
            sine[:, first : first + pairs] = -np.sin(angle)
            sine[:, first + pairs : first + 2 * pairs] = np.sin(angle)
        tables += [cosine, sine]
    return tables


def kernel(
    perm_hbm, tab_hbm, tok, wqkv, wout, out,
    perm, tab, xg, wq, wo, acc, cost, sint, swap, okv, oq, kv, qb, num, den,
    os1, or1, os2, or2, oss, ors, attn, zs1, zr1, zp, own, zs2, zr2, mixed,
    lsem, gs, gr, xs, xr, o1s, o1r, o2s, o2r, oqs, oqr, z1s, z1r, z2s, z2r,
):
    ctx = lax.axis_index("ctx")
    z = lax.axis_index("head")
    c = ctx % 2
    x = (ctx // 2) % N
    y = ctx // (2 * N)

    def cid(yy, xx, cc):
        return (yy * N + xx) * 2 + cc

    def kv_to(half, d):
        if half == 0:
            return cid(y, (x + d) % N, 0)
        return cid((y + d) % N, x, 1)

    def q_to(half, d):
        if half == 0:
            return cid((y + d) % N, x, 0)
        return cid(y, (x + d) % N, 1)

    def my_kv(d):
        return cid((y + c * d) % N, (x + (1 - c) * d) % N, c)

    def my_q(d, core):
        return cid((y + (1 - c) * d) % N, (x + c * d) % N, core)

    sibling = cid(y, x, 1 - c)
    kc = x * (1 - c) + y * c
    qc = y * (1 - c) + x * c

    def send(src, dst, ss, rs, to_ctx, to_z):
        pltpu.make_async_remote_copy(
            src_ref=src, dst_ref=dst, send_sem=ss, recv_sem=rs,
            device_id=(to_ctx, to_z), device_id_type=pl.DeviceIdType.MESH,
        ).start()

    def sized(ref, sem):
        return pltpu.make_async_remote_copy(
            src_ref=ref, dst_ref=ref, send_sem=sem, recv_sem=sem,
            device_id=(sibling, z), device_id_type=pl.DeviceIdType.MESH,
        )

    def arrive(dst, rs):
        sized(dst, rs).wait_recv()

    def left_here(src, ss):
        sized(src, ss).wait_send()

    perm_in = pltpu.make_async_copy(perm_hbm, perm, lsem.at[7])
    perm_in.start()
    tab_in = pltpu.make_async_copy(tab_hbm, tab, lsem.at[8])
    tab_in.start()
    tok_in = [
        pltpu.make_async_copy(tok.at[pl.ds(h * R, R)], xg.at[h, z], lsem.at[h]) for h in range(2)
    ]
    for copy in tok_in:
        copy.start()
    w_in = []
    for at, rel in enumerate((0, 3, 1, 2)):
        rows = pl.ds(pl.multiple_of((z + rel) % N * DW, DW), DW)
        w_in.append(pltpu.make_async_copy(wqkv.at[:, rows], wq.at[:, rows], lsem.at[2 + at]))
    for copy in w_in:
        copy.start()
    wo_in = pltpu.make_async_copy(wout, wo, lsem.at[6])
    wo_in.start()

    barrier = pltpu.get_barrier_semaphore()
    peers = [(sibling, z)]
    for d in STEP:
        peers.append((ctx, (z + d) % N))
        for core in range(2):
            peers.append((cid(y, (x + d) % N, core), z))
            peers.append((cid((y + d) % N, x, core), z))
    for peer in peers:
        pl.semaphore_signal(barrier, inc=1, device_id=peer, device_id_type=pl.DeviceIdType.MESH)
    pl.semaphore_wait(barrier, len(peers))

    half_rows = (pl.ds(0, R // 2), pl.ds(R // 2, R // 2))

    def halves(chunk):
        h, first, count, at = chunk
        return pl.ds(first, count // 2), pl.ds(first + count // 2, count // 2)

    def gather_own(chunk, turn):
        h, _, _, at = chunk
        for way in (RIGHT, LEFT):
            block = xg.at[h, z, halves(chunk)[way ^ turn]]
            got = gr.at[at, 1 + way if turn else 0]
            send(block, block, gs.at[at], got, ctx, (z + STEP[way]) % N)

    def gather_relay(chunk):
        h, first, count, at = chunk
        arrive(xg.at[h, z, pl.ds(first, count)], gr.at[at, 0])
        for way in (RIGHT, LEFT):
            block = xg.at[h, (z + N - STEP[way]) % N, halves(chunk)[way]]
            send(block, block, gs.at[at], gr.at[at, 3], ctx, (z + STEP[way]) % N)

    def gather_rest(chunk, way):
        h, _, _, at = chunk
        arrive(xg.at[h, (z + N - STEP[way]) % N, halves(chunk)[1 - way]], gr.at[at, 1 + way])

    def gather_last(chunk):
        h, first, count, at = chunk
        arrive(xg.at[h, (z + 2) % N, pl.ds(first, count)], gr.at[at, 3])

    def weights(at):
        w_in[at].wait()

    def project_own():
        rows = pl.ds(pl.multiple_of(z * DW, DW), DW)

        def tile(j, carry):
            at = pl.ds(pl.multiple_of(j * DW, DW), DW)
            a = jnp.concatenate([xg[h, z] for h in range(2)], axis=0)
            part = jnp.dot(a, wq[j, rows, :], preferred_element_type=F32)
            for h in range(2):
                acc[h, :, at] = part[h * R : (h + 1) * R]
            return carry

        lax.fori_loop(0, 3, tile, 0)

    def project(chunk, rel):
        h, first, count, _ = chunk
        src = (z + rel) % N
        rows = pl.ds(pl.multiple_of(src * DW, DW), DW)
        mine = pl.ds(first, count)

        def tile(j, carry):
            at = pl.ds(pl.multiple_of(j * DW, DW), DW)
            acc[h, mine, at] += jnp.dot(
                xg[h, src, mine], wq[j, rows, :], preferred_element_type=F32
            )
            return carry

        lax.fori_loop(0, 3, tile, 0)

    def tables():
        perm_in.wait()
        tab_in.wait()
        for s in range(4):
            at = perm[4 * ctx + s]
            rows = pl.ds(s * WW, WW)
            cost[rows, :] = tab[pl.ds(at, 1), :] + tab[pl.ds(256, WW), :]
            sint[rows, :] = tab[pl.ds(128 + at, 1), :] + tab[pl.ds(256 + WW, WW), :]
        source = lax.broadcasted_iota(jnp.int32, (2 * HD, 2 * HD), 0)
        target = lax.broadcasted_iota(jnp.int32, (2 * HD, 2 * HD), 1)
        lane = target % HD
        distance = jnp.where(lane < 16, 8, 28)
        low = (lane < 8) | ((lane >= 16) & (lane < 44)) | ((lane >= 72) & (lane < 100))
        partner = target + jnp.where(low, distance, -distance)
        swap[...] = jnp.where(source == partner, 1.0, 0.0).astype(BF)

    def finish(chunk):
        h, first, count, _ = chunk
        mine = pl.ds(first, count)
        cosine = cost[pl.ds(h * R + first, count), :]
        sine = sint[pl.ds(h * R + first, count), :]
        for j in range(2):
            pairs = [acc[h, mine, pl.ds(j * DW + i * 2 * HD, 2 * HD)] for i in range(HH)]
            stacked = jnp.concatenate([p.astype(BF) for p in pairs], axis=0)
            other = jnp.dot(stacked, swap[...], preferred_element_type=F32)
            for head in range(2 * HH):
                cols = slice(head % 2 * HD, (head % 2 + 1) * HD)
                v = pairs[head // 2][:, cols]
                w = other[head // 2 * count : (head // 2 + 1) * count, cols]
                square = jnp.mean(v * v, axis=-1, keepdims=True)
                factor = lax.rsqrt(square + EPSILON)
                if j == 0:
                    factor = factor * (HD**-0.5 / math.log(2.0))
                turned = ((v * cosine + w * sine) * factor).astype(BF)
                half, to = head // HH, pl.ds(head % HH * HD, HD)
                if j == 0:
                    oq[half, h, mine, to] = turned
                else:
                    okv[half, h, 0, mine, to] = turned
        for half in range(2):
            okv[half, h, 1, mine] = acc[h, mine, pl.ds(2 * DW + half * HW, HW)].astype(BF)

    def spread(chunk):
        h, first, count, at = chunk
        rows = pl.ds(first, count)
        for turn in range(2):
            for half in range(2):
                qslot = (y, x)[half]
                for way in (RIGHT, LEFT):
                    part = halves(chunk)[way ^ turn]
                    src, dst = oq.at[half, h, part], qb.at[h, qslot, c, part]
                    send(src, dst, xs.at[at, 0], xr.at[at, turn], q_to(half, STEP[way]), z)
        send(
            oq.at[1 - c, h, rows], qb.at[h, kc, c, rows], xs.at[at, 2], xr.at[at, 2], sibling, z
        )
        qb[h, qc, c, rows] = oq[c, h, rows]
        for turn in range(2):
            for half in range(2):
                kslot = (x, y)[half]
                for way in (RIGHT, LEFT):
                    part = way ^ turn
                    src, dst = okv.at[half, h, part, rows], kv.at[h, kslot, c, part, rows]
                    send(src, dst, xs.at[at, 0], xr.at[at, 4 + turn], kv_to(half, STEP[way]), z)
        send(
            okv.at[1 - c, h, :, rows], kv.at[h, qc, c, :, rows],
            xs.at[at, 3], xr.at[at, 6], sibling, z,
        )
        kv[h, kc, c, :, rows] = okv[c, h, :, rows]

    def spread_relay_q(chunk):
        h, first, count, at = chunk
        arrive(qb.at[h, qc, :, pl.ds(first, count)], xr.at[at, 0])
        for way in (RIGHT, LEFT):
            for core in range(2):
                block = qb.at[h, (qc + N - STEP[way]) % N, core, halves(chunk)[way]]
                send(block, block, xs.at[at, 1], xr.at[at, 3], my_q(STEP[way], c), z)

    def spread_relay_kv(chunk):
        h, first, count, at = chunk
        arrive(kv.at[h, kc, :, :, pl.ds(first, count)], xr.at[at, 4])
        for way in (RIGHT, LEFT):
            for core in range(2):
                block = kv.at[h, (kc + N - STEP[way]) % N, core, way, pl.ds(first, count)]
                send(block, block, xs.at[at, 1], xr.at[at, 7], my_kv(STEP[way]), z)

    def spread_sibling_q(chunk):
        h, first, count, at = chunk
        arrive(qb.at[h, qc, 1 - c, pl.ds(first, count)], xr.at[at, 2])

    def spread_rest_q(chunk):
        h, first, count, at = chunk
        arrive(qb.at[h, qc, :, pl.ds(first, count)], xr.at[at, 1])

    def spread_rest_kv(chunk):
        h, first, count, at = chunk
        arrive(kv.at[h, kc, 1 - c, :, pl.ds(first, count)], xr.at[at, 6])
        arrive(kv.at[h, kc, :, :, pl.ds(first, count)], xr.at[at, 5])

    def spread_last_q(chunk):
        h, first, count, at = chunk
        arrive(qb.at[h, (qc + 2) % N, :, pl.ds(first, count)], xr.at[at, 3])

    def spread_last_kv(chunk):
        h, first, count, at = chunk
        arrive(kv.at[h, (kc + 2) % N, :, :, pl.ds(first, count)], xr.at[at, 7])

    frame_rows = perm.shape[0] // 8

    def attend(queries, against):
        rows = [(h, (qc + rel) % N, a, first) for h, rel, first in queries for a in range(2)]
        keys = [(h, (kc + rel) % N, b) for h, rel in against for b in range(2)]
        fq = [
            perm[4 * cid((1 - c) * t + c * y, (1 - c) * x + c * t, a) + 2 * h] // frame_rows
            for h, t, a, _ in rows
        ]
        fk = [
            perm[4 * cid((1 - c) * y + c * t, (1 - c) * t + c * x, b) + 2 * h] // frame_rows
            for h, t, b in keys
        ]

        def seen(w, n, m):
            block = w[n * R : (n + 1) * R, m * R : (m + 1) * R]
            return block * (fk[m] <= fq[n]).astype(F32) if rows[n][0] == keys[m][0] else block

        for i in range(HH):
            cols = pl.ds(i * HD, HD)
            q = jnp.concatenate([qb[h, t, a, :, cols] for h, t, a, _ in rows], axis=0)
            k = jnp.concatenate([kv[h, t, b, 0, :, cols] for h, t, b in keys], axis=0)
            v = jnp.concatenate([kv[h, t, b, 1, :, cols] for h, t, b in keys], axis=0)
            s = lax.dot_general(q, k, (((1,), (1,)), ((), ())), preferred_element_type=F32)
            w = jnp.exp2(s)
            w = jnp.concatenate(
                [
                    jnp.concatenate([seen(w, n, m) for m in range(len(keys))], axis=1)
                    for n in range(len(rows))
                ],
                axis=0,
            )
            total = w[:, :HD]
            for b in range(1, len(keys)):
                total = total + w[:, b * HD : (b + 1) * HD]
            o = jnp.dot(w.astype(BF), v, preferred_element_type=F32)
            for n, (h, t, a, first) in enumerate(rows):
                piece = slice(n * R, (n + 1) * R)
                if first:
                    num[h, t, a, :, cols] = o[piece]
                    den[h, t, a, :, cols] = total[piece]
                else:
                    num[h, t, a, :, cols] += o[piece]
                    den[h, t, a, :, cols] += total[piece]

    def row_sum(h, slot, core, i):
        return jnp.sum(den[h, slot, core, :, pl.ds(i * HD, HD)].T, axis=0, keepdims=True)

    def pack(dst, h, slot, core, plus=None):
        for i in range(HH):
            cols = pl.ds(i * HD, HD)
            n = num[h, slot, core, :, cols]
            d = row_sum(h, slot, core, i)
            if plus is not None:
                n = n + plus[pl.ds(0, R), cols].astype(F32)
                d = d + plus[pl.ds(R, 8), cols].astype(F32)
            dst[pl.ds(0, R), cols] = n.astype(BF)
            dst[pl.ds(R, 8), cols] = jnp.broadcast_to(d, (8, HD)).astype(BF)

    def sum_far(h):
        far = (qc + 2) % N
        for way in (RIGHT, LEFT):
            pack(os1.at[h, way], h, far, way)
            send(os1.at[h, way], or1.at[h, way], o1s.at[h], o1r.at[h], my_q(STEP[way], c), z)

    def sum_near(h, way, core, plus=None):
        pack(os2.at[h, way, core], h, (qc + STEP[way]) % N, core, plus)
        dst = or2.at[h, c, way]
        send(os2.at[h, way, core], dst, o2s.at[h], o2r.at[h], my_q(STEP[way], core), z)

    def sum_plain(h, way):
        sum_near(h, way, 1 - way)

    def sum_passed(h):
        arrive(or1.at[h], o1r.at[h])
        for way in (RIGHT, LEFT):
            sum_near(h, way, way, or1.at[h, way])

    def sum_sibling(h):
        pack(oss.at[h], h, qc, 1 - c)
        send(oss.at[h], ors.at[h], oqs.at[h], oqr.at[h], sibling, z)

    def normalize(h):
        arrive(or2.at[h], o2r.at[h])
        arrive(ors.at[h], oqr.at[h])
        for mine in range(2):
            half = c if mine else 1 - c
            for i in range(HH):
                cols = pl.ds(i * HD, HD)
                if mine:
                    n = num[h, qc, c, :, cols]
                    d = row_sum(h, qc, c, i)
                else:
                    n = ors[h, pl.ds(0, R), cols].astype(F32)
                    d = ors[h, pl.ds(R, 8), cols].astype(F32)[:1]
                for way in (RIGHT, LEFT):
                    n = n + or2[h, half, way, pl.ds(0, R), cols].astype(F32)
                    d = d + or2[h, half, way, pl.ds(R, 8), cols].astype(F32)[:1]
                attn[h, half, :, cols] = (n / jnp.broadcast_to(d, (HD, R)).T).astype(BF)

    def mixed_for(h, rel, store):
        base = (z + rel) % N * DW

        for t in range(3):
            cols = pl.ds(pl.multiple_of(base + t * 256, 256), 256)
            part = jnp.dot(attn[h, 0], wo[pl.ds(0, HW), cols], preferred_element_type=F32)
            part += jnp.dot(attn[h, 1], wo[pl.ds(HW, HW), cols], preferred_element_type=F32)
            store(pl.ds(t * 256, 256), part)

    def mix_far(h):
        def store(cols, part):
            for way in (RIGHT, LEFT):
                zs1[h, way, :, cols] = part[way * (R // 2) : (way + 1) * (R // 2)].astype(BF)

        mixed_for(h, 2, store)
        for way in (RIGHT, LEFT):
            send(zs1.at[h, way], zr1.at[h, way], z1s.at[h], z1r.at[h], ctx, (z + STEP[way]) % N)

    def mix_send(h, way, part):
        src, dst = zs2.at[h, way, part], zr2.at[h, way, part]
        send(src, dst, z2s.at[h], z2r.at[h], ctx, (z + STEP[way]) % N)

    def mix_plain(h, way):
        part = 1 - way

        def store(cols, rows):
            zp[h, way, :, cols] = rows[way * (R // 2) : (way + 1) * (R // 2)]
            zs2[h, way, part, :, cols] = rows[part * (R // 2) : (part + 1) * (R // 2)].astype(BF)

        mixed_for(h, STEP[way], store)
        mix_send(h, way, part)

    def mix_own(h):
        def store(cols, rows):
            own[h, :, cols] = rows

        mixed_for(h, 0, store)

    def mix_passed(h):
        arrive(zr1.at[h], z1r.at[h])
        for way in (RIGHT, LEFT):
            zs2[h, way, way] = (zp[h, way] + zr1[h, way].astype(F32)).astype(BF)
            mix_send(h, way, way)

    def mix_last(h):
        arrive(zr2.at[h], z2r.at[h])
        for part in range(2):
            total = own[h, half_rows[part], :]
            for way in (RIGHT, LEFT):
                total = total + zr2[h, way, part].astype(F32)
            mixed[h, half_rows[part], :] = total.astype(BF)
        copy = pltpu.make_async_copy(mixed.at[h], out.at[pl.ds(h * R, R)], lsem.at[h])
        copy.start()
        outgoing.append(copy)

    near = (1, 3, 0)
    early = [(EARLY, rel) for rel in (1, 3, 0, 2)]
    late = [(LATE, rel) for rel in (1, 3, 0, 2)]
    outgoing = []
    tok_in[0].wait()
    gather_own(C0, 0)
    gather_own(C0, 1)
    gather_own(C1, 0)
    tables()
    tok_in[1].wait()
    weights(0)
    project_own()
    gather_relay(C0)
    gather_own(C1, 1)
    weights(1)
    gather_rest(C0, RIGHT)
    project(C0, 3)
    gather_relay(C1)
    gather_own(C2, 0)
    gather_own(C2, 1)
    weights(2)
    gather_rest(C0, LEFT)
    project(C0, 1)
    weights(3)
    gather_last(C0)
    project(C0, 2)
    finish(C0)
    spread(C0)
    gather_rest(C1, RIGHT)
    project(C1, 3)
    gather_rest(C1, LEFT)
    project(C1, 1)
    gather_last(C1)
    project(C1, 2)
    gather_relay(C2)
    finish(C1)
    spread(C1)
    spread_relay_q(C0)
    spread_relay_kv(C0)
    gather_rest(C2, RIGHT)
    project(C2, 3)
    gather_rest(C2, LEFT)
    project(C2, 1)
    gather_last(C2)
    project(C2, 2)
    finish(C2)
    spread_relay_q(C1)
    spread_relay_kv(C1)
    spread(C2)
    spread_sibling_q(C0)
    spread_sibling_q(C1)
    spread_rest_q(C0)
    spread_rest_q(C1)
    spread_rest_kv(C0)
    spread_rest_kv(C1)
    attend([(EARLY, rel, True) for rel in near], early[:3])
    spread_sibling_q(C2)
    spread_last_q(C0)
    spread_last_q(C1)
    attend([(EARLY, 2, True), (LATE, 0, True)], early[:3])
    spread_relay_q(C2)
    spread_last_kv(C0)
    spread_last_kv(C1)
    attend([(EARLY, rel, False) for rel in (1, 3, 0, 2)] + [(LATE, 0, False)], early[3:])
    sum_far(0)
    spread_rest_q(C2)
    attend([(LATE, 1, True), (LATE, 3, True)], early)
    spread_relay_kv(C2)
    sum_plain(0, RIGHT)
    sum_plain(0, LEFT)
    sum_sibling(0)
    spread_rest_kv(C2)
    attend([(LATE, rel, False) for rel in near], late[:3])
    sum_passed(0)
    spread_last_q(C2)
    attend([(LATE, 2, True)], early + late[:3])
    spread_last_kv(C2)
    attend([(LATE, 2, False)], late[3:])
    sum_far(1)
    attend([(LATE, rel, False) for rel in near], late[3:])
    sum_plain(1, RIGHT)
    sum_plain(1, LEFT)
    sum_sibling(1)
    wo_in.wait()
    normalize(0)
    mix_far(0)
    mix_plain(0, RIGHT)
    mix_plain(0, LEFT)
    sum_passed(1)
    mix_own(0)
    mix_passed(0)
    normalize(1)
    mix_far(1)
    mix_plain(1, RIGHT)
    mix_plain(1, LEFT)
    mix_own(1)
    mix_last(0)
    mix_passed(1)
    mix_last(1)
    for h, first, count, at in (C0, C1, C2):
        rows = pl.ds(first, count)
        left_here(xg.at[h, pl.ds(0, 3), rows], gs.at[at])
        left_here(kv.at[h, pl.ds(0, 3), :, :, rows], xs.at[at, 0])
        left_here(qb.at[h, pl.ds(0, 3), :, rows], xs.at[at, 1])
        left_here(oq.at[1 - c, h, rows], xs.at[at, 2])
        left_here(okv.at[1 - c, h, :, rows], xs.at[at, 3])
    for h in range(2):
        left_here(os1.at[h], o1s.at[h])
        left_here(os2.at[h], o2s.at[h])
        left_here(oss.at[h], oqs.at[h])
        left_here(zs1.at[h], z1s.at[h])
        left_here(zs2.at[h], z2s.at[h])
    for copy in outgoing:
        copy.wait()


def per_device(tokens, w_qkv, w_out, block_perm):
    table = jnp.asarray(np.concatenate(rope_tables(block_perm.shape[0] // 8)))
    hbm = pl.BlockSpec(memory_space=pl.ANY)
    dma = pltpu.SemaphoreType.DMA
    return pl.pallas_call(
        kernel,
        name="attention_layer",
        out_shape=jax.ShapeDtypeStruct((2 * R, DW), BF),
        in_specs=[hbm] * 5,
        out_specs=hbm,
        scratch_shapes=[
            pltpu.SMEM(block_perm.shape, jnp.int32),
            pltpu.VMEM(table.shape, F32),
            pltpu.VMEM((2, N, R, DW), BF),
            pltpu.VMEM((3, N * DW, DW), BF),
            pltpu.VMEM((DW, N * DW), BF),
            pltpu.VMEM((2, R, 3 * DW), F32),
            pltpu.VMEM((2 * R, HD), F32),
            pltpu.VMEM((2 * R, HD), F32),
            pltpu.VMEM((2 * HD, 2 * HD), BF),
            pltpu.VMEM((2, 2, 2, R, HW), BF),
            pltpu.VMEM((2, 2, R, HW), BF),
            pltpu.VMEM((2, N, 2, 2, R, HW), BF),
            pltpu.VMEM((2, N, 2, R, HW), BF),
            pltpu.VMEM((2, N, 2, R, HW), F32),
            pltpu.VMEM((2, N, 2, R, HW), F32),
            pltpu.VMEM((2, 2, OB, HW), BF),
            pltpu.VMEM((2, 2, OB, HW), BF),
            pltpu.VMEM((2, 2, 2, OB, HW), BF),
            pltpu.VMEM((2, 2, 2, OB, HW), BF),
            pltpu.VMEM((2, OB, HW), BF),
            pltpu.VMEM((2, OB, HW), BF),
            pltpu.VMEM((2, 2, R, HW), BF),
            pltpu.VMEM((2, 2, R // 2, DW), BF),
            pltpu.VMEM((2, 2, R // 2, DW), BF),
            pltpu.VMEM((2, 2, R // 2, DW), F32),
            pltpu.VMEM((2, R, DW), F32),
            pltpu.VMEM((2, 2, 2, R // 2, DW), BF),
            pltpu.VMEM((2, 2, 2, R // 2, DW), BF),
            pltpu.VMEM((2, R, DW), BF),
            dma((9,)),
            dma((3,)),
            dma((3, 4)),
            dma((3, 4)),
            dma((3, 8)),
            dma((2,)),
            dma((2,)),
            dma((2,)),
            dma((2,)),
            dma((2,)),
            dma((2,)),
            dma((2,)),
            dma((2,)),
            dma((2,)),
            dma((2,)),
        ],
        compiler_params=pltpu.CompilerParams(
            collective_id=0, has_side_effects=True, vmem_limit_bytes=64 * 1024 * 1024 - 65536
        ),
    )(block_perm, table, tokens, w_qkv, w_out)


def solution(mesh):
    in_specs = (P("ctx", "head"), P(None, None, "head"), P("head", None), P())
    return jax.shard_map(
        per_device, mesh=mesh, in_specs=in_specs, out_specs=P("ctx", "head"), check_vma=False
    )
```

```python
import functools
import math

import jax
import jax.numpy as jnp
import numpy as np
from jax import lax
from jax.experimental import pallas as pl
from jax.experimental.pallas import tpu as pltpu
from jax.sharding import PartitionSpec as P

HD = 128
WW = 64
ROPE_BASE = 10000.0
EPSILON = 1e-06
N = 4
R = 128
HH = 3
HW = HH * HD
DW = 2 * HW
OB = R + 8
BF = jnp.bfloat16
F32 = jnp.float32
RIGHT, LEFT = 0, 1
EARLY, LATE = 0, 1
C0, C1, C2 = (EARLY, 0, R // 2, 0), (EARLY, R // 2, R // 2, 1), (LATE, 0, R, 2)
STEP = (1, N - 1)


def rope_tables(frame_rows):
    parts = ((0, HD // 16), (HD // 8, 7 * HD // 32), (HD // 8 + 7 * HD // 16, 7 * HD // 32))
    frames = np.arange(128) // frame_rows
    rows = np.arange(128) % frame_rows
    tables = []
    for position, kinds in ((np.stack([frames, rows]), (0, 1)), (np.arange(WW)[None], (2,))):
        cosine = np.zeros((position.shape[1], HD), np.float32)
        sine = np.zeros((position.shape[1], HD), np.float32)
        for at, kind in enumerate(kinds):
            first, pairs = parts[kind]
            freq = np.float32(ROPE_BASE) ** (-np.arange(pairs, dtype=np.float32) / pairs)
            angle = position[at].astype(np.float32)[:, None] * freq[None, :].astype(np.float32)
            cosine[:, first : first + pairs] = np.cos(angle)
            cosine[:, first + pairs : first + 2 * pairs] = np.cos(angle)
            sine[:, first : first + pairs] = -np.sin(angle)
            sine[:, first + pairs : first + 2 * pairs] = np.sin(angle)
        tables += [cosine, sine]
    return tables


def kernel(
    perm_hbm, tab_hbm, tok, wqkv, wout, out,
    perm, tab, xg, wq, wo, acc, cost, sint, swap, okv, oq, kv, qb, num, den,
    os1, or1, os2, or2, oss, ors, attn, zs1, zr1, zp, own, zs2, zr2, mixed,
    lsem, gs, gr, xs, xr, o1s, o1r, o2s, o2r, oqs, oqr, z1s, z1r, z2s, z2r,
):
    ctx = lax.axis_index("ctx")
    z = lax.axis_index("head")
    c = ctx % 2
    x = (ctx // 2) % N
    y = ctx // (2 * N)

    def cid(yy, xx, cc):
        return (yy * N + xx) * 2 + cc

    def kv_to(half, d):
        if half == 0:
            return cid(y, (x + d) % N, 0)
        return cid((y + d) % N, x, 1)

    def q_to(half, d):
        if half == 0:
            return cid((y + d) % N, x, 0)
        return cid(y, (x + d) % N, 1)

    def my_kv(d):
        return cid((y + c * d) % N, (x + (1 - c) * d) % N, c)

    def my_q(d, core):
        return cid((y + (1 - c) * d) % N, (x + c * d) % N, core)

    sibling = cid(y, x, 1 - c)
    kc = x * (1 - c) + y * c
    qc = y * (1 - c) + x * c

    def send(src, dst, ss, rs, to_ctx, to_z):
        pltpu.make_async_remote_copy(
            src_ref=src, dst_ref=dst, send_sem=ss, recv_sem=rs,
            device_id=(to_ctx, to_z), device_id_type=pl.DeviceIdType.MESH,
        ).start()

    def sized(ref, sem):
        return pltpu.make_async_remote_copy(
            src_ref=ref, dst_ref=ref, send_sem=sem, recv_sem=sem,
            device_id=(sibling, z), device_id_type=pl.DeviceIdType.MESH,
        )

    def arrive(dst, rs):
        sized(dst, rs).wait_recv()

    def left_here(src, ss):
        sized(src, ss).wait_send()

    perm_in = pltpu.make_async_copy(perm_hbm, perm, lsem.at[7])
    perm_in.start()
    tab_in = pltpu.make_async_copy(tab_hbm, tab, lsem.at[8])
    tab_in.start()
    tok_in = [
        pltpu.make_async_copy(tok.at[pl.ds(h * R, R)], xg.at[h, z], lsem.at[h]) for h in range(2)
    ]
    for copy in tok_in:
        copy.start()
    w_in = []
    for at, rel in enumerate((0, 3, 1, 2)):
        rows = pl.ds(pl.multiple_of((z + rel) % N * DW, DW), DW)
        w_in.append(pltpu.make_async_copy(wqkv.at[:, rows], wq.at[:, rows], lsem.at[2 + at]))
    for copy in w_in:
        copy.start()
    wo_in = pltpu.make_async_copy(wout, wo, lsem.at[6])
    wo_in.start()

    barrier = pltpu.get_barrier_semaphore()
    peers = [(sibling, z)]
    for d in STEP:
        peers.append((ctx, (z + d) % N))
        for core in range(2):
            peers.append((cid(y, (x + d) % N, core), z))
            peers.append((cid((y + d) % N, x, core), z))
    for peer in peers:
        pl.semaphore_signal(barrier, inc=1, device_id=peer, device_id_type=pl.DeviceIdType.MESH)
    pl.semaphore_wait(barrier, len(peers))

    half_rows = (pl.ds(0, R // 2), pl.ds(R // 2, R // 2))

    def halves(chunk):
        h, first, count, at = chunk
        return pl.ds(first, count // 2), pl.ds(first + count // 2, count // 2)

    def gather_own(chunk, turn):
        h, _, _, at = chunk
        for way in (RIGHT, LEFT):
            block = xg.at[h, z, halves(chunk)[way ^ turn]]
            got = gr.at[at, 1 + way if turn else 0]
            send(block, block, gs.at[0], got, ctx, (z + STEP[way]) % N)

    def gather_relay(chunk):
        h, first, count, at = chunk
        arrive(xg.at[h, z, pl.ds(first, count)], gr.at[at, 0])
        for way in (RIGHT, LEFT):
            block = xg.at[h, (z + N - STEP[way]) % N, halves(chunk)[way]]
            send(block, block, gs.at[0], gr.at[at, 3], ctx, (z + STEP[way]) % N)

    def gather_rest(chunk, way):
        h, _, _, at = chunk
        arrive(xg.at[h, (z + N - STEP[way]) % N, halves(chunk)[1 - way]], gr.at[at, 1 + way])

    def gather_last(chunk):
        h, first, count, at = chunk
        arrive(xg.at[h, (z + 2) % N, pl.ds(first, count)], gr.at[at, 3])

    def weights(at):
        w_in[at].wait()

    def project_own():
        rows = pl.ds(pl.multiple_of(z * DW, DW), DW)

        def tile(j, carry):
            at = pl.ds(pl.multiple_of(j * DW, DW), DW)
            a = jnp.concatenate([xg[h, z] for h in range(2)], axis=0)
            part = jnp.dot(a, wq[j, rows, :], preferred_element_type=F32)
            for h in range(2):
                acc[h, :, at] = part[h * R : (h + 1) * R]
            return carry

        lax.fori_loop(0, 3, tile, 0)

    def project(chunk, rel):
        h, first, count, _ = chunk
        src = (z + rel) % N
        rows = pl.ds(pl.multiple_of(src * DW, DW), DW)
        mine = pl.ds(first, count)

        def tile(j, carry):
            at = pl.ds(pl.multiple_of(j * DW, DW), DW)
            acc[h, mine, at] += jnp.dot(
                xg[h, src, mine], wq[j, rows, :], preferred_element_type=F32
            )
            return carry

        lax.fori_loop(0, 3, tile, 0)

    def tables():
        perm_in.wait()
        tab_in.wait()
        for s in range(4):
            at = perm[4 * ctx + s]
            rows = pl.ds(s * WW, WW)
            cost[rows, :] = tab[pl.ds(at, 1), :] + tab[pl.ds(256, WW), :]
            sint[rows, :] = tab[pl.ds(128 + at, 1), :] + tab[pl.ds(256 + WW, WW), :]
        source = lax.broadcasted_iota(jnp.int32, (2 * HD, 2 * HD), 0)
        target = lax.broadcasted_iota(jnp.int32, (2 * HD, 2 * HD), 1)
        lane = target % HD
        distance = jnp.where(lane < 16, 8, 28)
        low = (lane < 8) | ((lane >= 16) & (lane < 44)) | ((lane >= 72) & (lane < 100))
        partner = target + jnp.where(low, distance, -distance)
        swap[...] = jnp.where(source == partner, 1.0, 0.0).astype(BF)

    def finish(chunk):
        h, first, count, _ = chunk
        mine = pl.ds(first, count)
        cosine = cost[pl.ds(h * R + first, count), :]
        sine = sint[pl.ds(h * R + first, count), :]
        for j in range(2):
            pairs = [acc[h, mine, pl.ds(j * DW + i * 2 * HD, 2 * HD)] for i in range(HH)]
            stacked = jnp.concatenate([p.astype(BF) for p in pairs], axis=0)
            other = jnp.dot(stacked, swap[...], preferred_element_type=F32)
            for head in range(2 * HH):
                cols = slice(head % 2 * HD, (head % 2 + 1) * HD)
                v = pairs[head // 2][:, cols]
                w = other[head // 2 * count : (head // 2 + 1) * count, cols]
                square = jnp.mean(v * v, axis=-1, keepdims=True)
                factor = lax.rsqrt(square + EPSILON)
                if j == 0:
                    factor = factor * (HD**-0.5 / math.log(2.0))
                turned = ((v * cosine + w * sine) * factor).astype(BF)
                half, to = head // HH, pl.ds(head % HH * HD, HD)
                if j == 0:
                    oq[half, h, mine, to] = turned
                else:
                    okv[half, h, 0, mine, to] = turned
        for half in range(2):
            okv[half, h, 1, mine] = acc[h, mine, pl.ds(2 * DW + half * HW, HW)].astype(BF)

    def spread(chunk):
        h, first, count, at = chunk
        rows = pl.ds(first, count)
        for turn in range(2):
            for half in range(2):
                qslot = (y, x)[half]
                for way in (RIGHT, LEFT):
                    part = halves(chunk)[way ^ turn]
                    src, dst = oq.at[half, h, part], qb.at[h, qslot, c, part]
                    send(src, dst, xs.at[0], xr.at[at, turn], q_to(half, STEP[way]), z)
        send(
            oq.at[1 - c, h, rows], qb.at[h, kc, c, rows], xs.at[2], xr.at[at, 2], sibling, z
        )
        qb[h, qc, c, rows] = oq[c, h, rows]
        for turn in range(2):
            for half in range(2):
                kslot = (x, y)[half]
                for way in (RIGHT, LEFT):
                    part = way ^ turn
                    src, dst = okv.at[half, h, part, rows], kv.at[h, kslot, c, part, rows]
                    send(src, dst, xs.at[0], xr.at[at, 4 + turn], kv_to(half, STEP[way]), z)
        send(
            okv.at[1 - c, h, :, rows], kv.at[h, qc, c, :, rows],
            xs.at[3], xr.at[at, 6], sibling, z,
        )
        kv[h, kc, c, :, rows] = okv[c, h, :, rows]

    def spread_relay_q(chunk):
        h, first, count, at = chunk
        arrive(qb.at[h, qc, :, pl.ds(first, count)], xr.at[at, 0])
        for way in (RIGHT, LEFT):
            for core in range(2):
                block = qb.at[h, (qc + N - STEP[way]) % N, core, halves(chunk)[way]]
                send(block, block, xs.at[1], xr.at[at, 3], my_q(STEP[way], c), z)

    def spread_relay_kv(chunk):
        h, first, count, at = chunk
        arrive(kv.at[h, kc, :, :, pl.ds(first, count)], xr.at[at, 4])
        for way in (RIGHT, LEFT):
            for core in range(2):
                block = kv.at[h, (kc + N - STEP[way]) % N, core, way, pl.ds(first, count)]
                send(block, block, xs.at[1], xr.at[at, 7], my_kv(STEP[way]), z)

    def spread_sibling_q(chunk):
        h, first, count, at = chunk
        arrive(qb.at[h, qc, 1 - c, pl.ds(first, count)], xr.at[at, 2])

    def spread_rest_q(chunk):
        h, first, count, at = chunk
        arrive(qb.at[h, qc, :, pl.ds(first, count)], xr.at[at, 1])

    def spread_rest_kv(chunk):
        h, first, count, at = chunk
        arrive(kv.at[h, kc, 1 - c, :, pl.ds(first, count)], xr.at[at, 6])
        arrive(kv.at[h, kc, :, :, pl.ds(first, count)], xr.at[at, 5])

    def spread_last_q(chunk):
        h, first, count, at = chunk
        arrive(qb.at[h, (qc + 2) % N, :, pl.ds(first, count)], xr.at[at, 3])

    def spread_last_kv(chunk):
        h, first, count, at = chunk
        arrive(kv.at[h, (kc + 2) % N, :, :, pl.ds(first, count)], xr.at[at, 7])

    frame_rows = perm.shape[0] // 8

    def attend(queries, against):
        rows = [(h, (qc + rel) % N, a, first) for h, rel, first in queries for a in range(2)]
        keys = [(h, (kc + rel) % N, b) for h, rel in against for b in range(2)]
        fq = [
            perm[4 * cid((1 - c) * t + c * y, (1 - c) * x + c * t, a) + 2 * h] // frame_rows
            for h, t, a, _ in rows
        ]
        fk = [
            perm[4 * cid((1 - c) * y + c * t, (1 - c) * t + c * x, b) + 2 * h] // frame_rows
            for h, t, b in keys
        ]

        def seen(w, n, m):
            block = w[n * R : (n + 1) * R, m * R : (m + 1) * R]
            return block * (fk[m] <= fq[n]).astype(F32) if rows[n][0] == keys[m][0] else block

        for i in range(HH):
            cols = pl.ds(i * HD, HD)
            q = jnp.concatenate([qb[h, t, a, :, cols] for h, t, a, _ in rows], axis=0)
            k = jnp.concatenate([kv[h, t, b, 0, :, cols] for h, t, b in keys], axis=0)
            v = jnp.concatenate([kv[h, t, b, 1, :, cols] for h, t, b in keys], axis=0)
            s = lax.dot_general(q, k, (((1,), (1,)), ((), ())), preferred_element_type=F32)
            w = jnp.exp2(s)
            w = jnp.concatenate(
                [
                    jnp.concatenate([seen(w, n, m) for m in range(len(keys))], axis=1)
                    for n in range(len(rows))
                ],
                axis=0,
            )
            total = w[:, :HD]
            for b in range(1, len(keys)):
                total = total + w[:, b * HD : (b + 1) * HD]
            o = jnp.dot(w.astype(BF), v, preferred_element_type=F32)
            for n, (h, t, a, first) in enumerate(rows):
                piece = slice(n * R, (n + 1) * R)
                if first:
                    num[h, t, a, :, cols] = o[piece]
                    den[h, t, a, :, cols] = total[piece]
                else:
                    num[h, t, a, :, cols] += o[piece]
                    den[h, t, a, :, cols] += total[piece]

    def row_sum(h, slot, core, i):
        return jnp.sum(den[h, slot, core, :, pl.ds(i * HD, HD)].T, axis=0, keepdims=True)

    def pack(dst, h, slot, core, plus=None):
        for i in range(HH):
            cols = pl.ds(i * HD, HD)
            n = num[h, slot, core, :, cols]
            d = row_sum(h, slot, core, i)
            if plus is not None:
                n = n + plus[pl.ds(0, R), cols].astype(F32)
                d = d + plus[pl.ds(R, 8), cols].astype(F32)
            dst[pl.ds(0, R), cols] = n.astype(BF)
            dst[pl.ds(R, 8), cols] = jnp.broadcast_to(d, (8, HD)).astype(BF)

    def sum_far(h):
        far = (qc + 2) % N
        for way in (RIGHT, LEFT):
            pack(os1.at[h, way], h, far, way)
            send(os1.at[h, way], or1.at[h, way], o1s.at[0], o1r.at[h], my_q(STEP[way], c), z)

    def sum_near(h, way, core, plus=None):
        pack(os2.at[h, way, core], h, (qc + STEP[way]) % N, core, plus)
        dst = or2.at[h, c, way]
        send(os2.at[h, way, core], dst, o2s.at[0], o2r.at[h], my_q(STEP[way], core), z)

    def sum_plain(h, way):
        sum_near(h, way, 1 - way)

    def sum_passed(h):
        arrive(or1.at[h], o1r.at[h])
        for way in (RIGHT, LEFT):
            sum_near(h, way, way, or1.at[h, way])

    def sum_sibling(h):
        pack(oss.at[h], h, qc, 1 - c)
        send(oss.at[h], ors.at[h], oqs.at[0], oqr.at[h], sibling, z)

    def normalize(h):
        arrive(or2.at[h], o2r.at[h])
        arrive(ors.at[h], oqr.at[h])
        for mine in range(2):
            half = c if mine else 1 - c
            for i in range(HH):
                cols = pl.ds(i * HD, HD)
                if mine:
                    n = num[h, qc, c, :, cols]
                    d = row_sum(h, qc, c, i)
                else:
                    n = ors[h, pl.ds(0, R), cols].astype(F32)
                    d = ors[h, pl.ds(R, 8), cols].astype(F32)[:1]
                for way in (RIGHT, LEFT):
                    n = n + or2[h, half, way, pl.ds(0, R), cols].astype(F32)
                    d = d + or2[h, half, way, pl.ds(R, 8), cols].astype(F32)[:1]
                attn[h, half, :, cols] = (n / jnp.broadcast_to(d, (HD, R)).T).astype(BF)

    def mixed_for(h, rel, store):
        base = (z + rel) % N * DW

        for t in range(3):
            cols = pl.ds(pl.multiple_of(base + t * 256, 256), 256)
            part = jnp.dot(attn[h, 0], wo[pl.ds(0, HW), cols], preferred_element_type=F32)
            part += jnp.dot(attn[h, 1], wo[pl.ds(HW, HW), cols], preferred_element_type=F32)
            store(pl.ds(t * 256, 256), part)

    def mix_far(h):
        def store(cols, part):
            for way in (RIGHT, LEFT):
                zs1[h, way, :, cols] = part[way * (R // 2) : (way + 1) * (R // 2)].astype(BF)
                src, dst = zs1.at[h, way, :, cols], zr1.at[h, way, :, cols]
                send(src, dst, z1s.at[0], z1r.at[h], ctx, (z + STEP[way]) % N)

        mixed_for(h, 2, store)

    def mix_send(h, way, part):
        src, dst = zs2.at[h, way, part], zr2.at[h, way, part]
        send(src, dst, z2s.at[0], z2r.at[h], ctx, (z + STEP[way]) % N)

    def mix_plain(h, way):
        part = 1 - way

        def store(cols, rows):
            zp[h, way, :, cols] = rows[way * (R // 2) : (way + 1) * (R // 2)]
            zs2[h, way, part, :, cols] = rows[part * (R // 2) : (part + 1) * (R // 2)].astype(BF)

        mixed_for(h, STEP[way], store)
        mix_send(h, way, part)

    def mix_own(h):
        def store(cols, rows):
            own[h, :, cols] = rows

        mixed_for(h, 0, store)

    def mix_passed(h):
        arrive(zr1.at[h], z1r.at[h])
        for way in (RIGHT, LEFT):
            zs2[h, way, way] = (zp[h, way] + zr1[h, way].astype(F32)).astype(BF)
            mix_send(h, way, way)

    def mix_last(h):
        arrive(zr2.at[h], z2r.at[h])
        for part in range(2):
            total = own[h, half_rows[part], :]
            for way in (RIGHT, LEFT):
                total = total + zr2[h, way, part].astype(F32)
            mixed[h, half_rows[part], :] = total.astype(BF)
        copy = pltpu.make_async_copy(mixed.at[h], out.at[pl.ds(h * R, R)], lsem.at[h])
        copy.start()
        outgoing.append(copy)

    near = (1, 3, 0)
    early = [(EARLY, rel) for rel in (1, 3, 0, 2)]
    late = [(LATE, rel) for rel in (1, 3, 0, 2)]
    outgoing = []
    tok_in[0].wait()
    gather_own(C0, 0)
    gather_own(C0, 1)
    gather_own(C1, 0)
    tables()
    tok_in[1].wait()
    weights(0)
    project_own()
    gather_relay(C0)
    gather_own(C1, 1)
    weights(1)
    gather_rest(C0, RIGHT)
    project(C0, 3)
    gather_relay(C1)
    gather_own(C2, 0)
    gather_own(C2, 1)
    weights(2)
    gather_rest(C0, LEFT)
    project(C0, 1)
    weights(3)
    gather_last(C0)
    project(C0, 2)
    finish(C0)
    spread(C0)
    gather_rest(C1, RIGHT)
    project(C1, 3)
    gather_rest(C1, LEFT)
    project(C1, 1)
    gather_last(C1)
    project(C1, 2)
    gather_relay(C2)
    finish(C1)
    spread(C1)
    gather_rest(C2, RIGHT)
    project(C2, 3)
    spread_relay_q(C0)
    spread_relay_kv(C0)
    gather_rest(C2, LEFT)
    project(C2, 1)
    gather_last(C2)
    spread_relay_q(C1)
    spread_relay_kv(C1)
    project(C2, 2)
    finish(C2)
    spread(C2)
    spread_sibling_q(C0)
    spread_sibling_q(C1)
    spread_rest_q(C0)
    spread_rest_q(C1)
    spread_rest_kv(C0)
    spread_rest_kv(C1)
    attend([(EARLY, rel, True) for rel in near], early[:3])
    spread_sibling_q(C2)
    attend([(LATE, 0, True)], early[:3])
    spread_last_q(C0)
    spread_last_q(C1)
    spread_last_kv(C0)
    spread_last_kv(C1)
    attend([(EARLY, 2, True)], early)
    spread_relay_q(C2)
    sum_far(0)
    attend([(EARLY, rel, False) for rel in near] + [(LATE, 0, False)], early[3:])
    spread_rest_q(C2)
    attend([(LATE, 1, True)], early)
    attend([(LATE, 3, True)], early)
    spread_relay_kv(C2)
    sum_plain(0, RIGHT)
    sum_plain(0, LEFT)
    sum_sibling(0)
    spread_rest_kv(C2)
    attend([(LATE, rel, False) for rel in near], late[:3])
    sum_passed(0)
    spread_last_q(C2)
    attend([(LATE, 2, True)], early + late[:3])
    spread_last_kv(C2)
    attend([(LATE, 2, False)], late[3:])
    sum_far(1)
    attend([(LATE, rel, False) for rel in near], late[3:])
    sum_plain(1, RIGHT)
    sum_plain(1, LEFT)
    sum_sibling(1)
    wo_in.wait()
    normalize(0)
    mix_far(0)
    mix_plain(0, RIGHT)
    mix_plain(0, LEFT)
    sum_passed(1)
    mix_own(0)
    mix_passed(0)
    normalize(1)
    mix_far(1)
    mix_plain(1, RIGHT)
    mix_plain(1, LEFT)
    mix_own(1)
    mix_last(0)
    mix_passed(1)
    mix_last(1)
    left_here(xg.at[:, pl.ds(0, 3)], gs.at[0])
    left_here(kv.at[:, pl.ds(0, 3)], xs.at[0])
    left_here(qb.at[:, pl.ds(0, 3)], xs.at[1])
    left_here(oq.at[1 - c], xs.at[2])
    left_here(okv.at[1 - c], xs.at[3])
    left_here(os1, o1s.at[0])
    left_here(os2, o2s.at[0])
    left_here(oss, oqs.at[0])
    left_here(zs1, z1s.at[0])
    left_here(zs2, z2s.at[0])
    for copy in outgoing:
        copy.wait()


def per_device(tokens, w_qkv, w_out, block_perm):
    table = jnp.asarray(np.concatenate(rope_tables(block_perm.shape[0] // 8)))
    hbm = pl.BlockSpec(memory_space=pl.ANY)
    dma = pltpu.SemaphoreType.DMA
    return pl.pallas_call(
        kernel,
        name="attention_layer",
        out_shape=jax.ShapeDtypeStruct((2 * R, DW), BF),
        in_specs=[hbm] * 5,
        out_specs=hbm,
        scratch_shapes=[
            pltpu.SMEM(block_perm.shape, jnp.int32),
            pltpu.VMEM(table.shape, F32),
            pltpu.VMEM((2, N, R, DW), BF),
            pltpu.VMEM((3, N * DW, DW), BF),
            pltpu.VMEM((DW, N * DW), BF),
            pltpu.VMEM((2, R, 3 * DW), F32),
            pltpu.VMEM((2 * R, HD), F32),
            pltpu.VMEM((2 * R, HD), F32),
            pltpu.VMEM((2 * HD, 2 * HD), BF),
            pltpu.VMEM((2, 2, 2, R, HW), BF),
            pltpu.VMEM((2, 2, R, HW), BF),
            pltpu.VMEM((2, N, 2, 2, R, HW), BF),
            pltpu.VMEM((2, N, 2, R, HW), BF),
            pltpu.VMEM((2, N, 2, R, HW), F32),
            pltpu.VMEM((2, N, 2, R, HW), F32),
            pltpu.VMEM((2, 2, OB, HW), BF),
            pltpu.VMEM((2, 2, OB, HW), BF),
            pltpu.VMEM((2, 2, 2, OB, HW), BF),
            pltpu.VMEM((2, 2, 2, OB, HW), BF),
            pltpu.VMEM((2, OB, HW), BF),
            pltpu.VMEM((2, OB, HW), BF),
            pltpu.VMEM((2, 2, R, HW), BF),
            pltpu.VMEM((2, 2, R // 2, DW), BF),
            pltpu.VMEM((2, 2, R // 2, DW), BF),
            pltpu.VMEM((2, 2, R // 2, DW), F32),
            pltpu.VMEM((2, R, DW), F32),
            pltpu.VMEM((2, 2, 2, R // 2, DW), BF),
            pltpu.VMEM((2, 2, 2, R // 2, DW), BF),
            pltpu.VMEM((2, R, DW), BF),
            dma((9,)),
            dma((1,)),
            dma((3, 4)),
            dma((4,)),
            dma((3, 8)),
            dma((1,)),
            dma((2,)),
            dma((1,)),
            dma((2,)),
            dma((1,)),
            dma((2,)),
            dma((1,)),
            dma((2,)),
            dma((1,)),
            dma((2,)),
        ],
        compiler_params=pltpu.CompilerParams(
            collective_id=0, has_side_effects=True, vmem_limit_bytes=64 * 1024 * 1024 - 65536
        ),
    )(block_perm, table, tokens, w_qkv, w_out)


def solution(mesh):
    in_specs = (P("ctx", "head"), P(None, None, "head"), P("head", None), P())
    return jax.shard_map(
        per_device, mesh=mesh, in_specs=in_specs, out_specs=P("ctx", "head"), check_vma=False
    )
```

```python
import functools
import math

import jax
import jax.numpy as jnp
import numpy as np
from jax import lax
from jax.experimental import pallas as pl
from jax.experimental.pallas import tpu as pltpu
from jax.sharding import PartitionSpec as P

HD = 128
WW = 64
ROPE_BASE = 10000.0
EPSILON = 1e-06
N = 4
R = 128
HH = 3
HW = HH * HD
DW = 2 * HW
OB = R + 8
BF = jnp.bfloat16
F32 = jnp.float32
RIGHT, LEFT = 0, 1
EARLY, LATE = 0, 1
C0, C1, C2 = (EARLY, 0, R // 2, 0), (EARLY, R // 2, R // 2, 1), (LATE, 0, R, 2)
STEP = (1, N - 1)


def rope_tables(frame_rows):
    parts = ((0, HD // 16), (HD // 8, 7 * HD // 32), (HD // 8 + 7 * HD // 16, 7 * HD // 32))
    frames = np.arange(128) // frame_rows
    rows = np.arange(128) % frame_rows
    tables = []
    for position, kinds in ((np.stack([frames, rows]), (0, 1)), (np.arange(WW)[None], (2,))):
        cosine = np.zeros((position.shape[1], HD), np.float32)
        sine = np.zeros((position.shape[1], HD), np.float32)
        for at, kind in enumerate(kinds):
            first, pairs = parts[kind]
            freq = np.float32(ROPE_BASE) ** (-np.arange(pairs, dtype=np.float32) / pairs)
            angle = position[at].astype(np.float32)[:, None] * freq[None, :].astype(np.float32)
            cosine[:, first : first + pairs] = np.cos(angle)
            cosine[:, first + pairs : first + 2 * pairs] = np.cos(angle)
            sine[:, first : first + pairs] = -np.sin(angle)
            sine[:, first + pairs : first + 2 * pairs] = np.sin(angle)
        tables += [cosine, sine]
    return tables


def kernel(
    perm_hbm, tab_hbm, tok, wqkv, wout, out,
    perm, tab, xg, wq, wo, acc, cost, sint, swap, okv, oq, kv, qb, num, den,
    os1, or1, os2, or2, oss, ors, attn, zs1, zr1, zp, own, zs2, zr2, mixed,
    lsem, gs, gr, xs, xr, o1s, o1r, o2s, o2r, oqs, oqr, z1s, z1r, z2s, z2r,
):
    ctx = lax.axis_index("ctx")
    z = lax.axis_index("head")
    c = ctx % 2
    x = (ctx // 2) % N
    y = ctx // (2 * N)

    def cid(yy, xx, cc):
        return (yy * N + xx) * 2 + cc

    def kv_to(half, d):
        if half == 0:
            return cid(y, (x + d) % N, 0)
        return cid((y + d) % N, x, 1)

    def q_to(half, d):
        if half == 0:
            return cid((y + d) % N, x, 0)
        return cid(y, (x + d) % N, 1)

    def my_kv(d):
        return cid((y + c * d) % N, (x + (1 - c) * d) % N, c)

    def my_q(d, core):
        return cid((y + (1 - c) * d) % N, (x + c * d) % N, core)

    sibling = cid(y, x, 1 - c)
    kc = x * (1 - c) + y * c
    qc = y * (1 - c) + x * c

    def send(src, dst, ss, rs, to_ctx, to_z):
        pltpu.make_async_remote_copy(
            src_ref=src, dst_ref=dst, send_sem=ss, recv_sem=rs,
            device_id=(to_ctx, to_z), device_id_type=pl.DeviceIdType.MESH,
        ).start()

    def sized(ref, sem):
        return pltpu.make_async_remote_copy(
            src_ref=ref, dst_ref=ref, send_sem=sem, recv_sem=sem,
            device_id=(sibling, z), device_id_type=pl.DeviceIdType.MESH,
        )

    def arrive(dst, rs):
        sized(dst, rs).wait_recv()

    def left_here(src, ss):
        sized(src, ss).wait_send()

    perm_in = pltpu.make_async_copy(perm_hbm, perm, lsem.at[7])
    perm_in.start()
    tab_in = pltpu.make_async_copy(tab_hbm, tab, lsem.at[8])
    tab_in.start()
    tok_in = [
        pltpu.make_async_copy(tok.at[pl.ds(h * R, R)], xg.at[h, z], lsem.at[h]) for h in range(2)
    ]
    for copy in tok_in:
        copy.start()
    w_in = []
    for at, rel in enumerate((0, 3, 1, 2)):
        rows = pl.ds(pl.multiple_of((z + rel) % N * DW, DW), DW)
        w_in.append(pltpu.make_async_copy(wqkv.at[:, rows], wq.at[:, rows], lsem.at[2 + at]))
    for copy in w_in:
        copy.start()
    wo_in = pltpu.make_async_copy(wout, wo, lsem.at[6])
    wo_in.start()

    barrier = pltpu.get_barrier_semaphore()
    peers = [(sibling, z)]
    for d in STEP:
        peers.append((ctx, (z + d) % N))
        for core in range(2):
            peers.append((cid(y, (x + d) % N, core), z))
            peers.append((cid((y + d) % N, x, core), z))
    for peer in peers:
        pl.semaphore_signal(barrier, inc=1, device_id=peer, device_id_type=pl.DeviceIdType.MESH)
    pl.semaphore_wait(barrier, len(peers))

    half_rows = (pl.ds(0, R // 2), pl.ds(R // 2, R // 2))

    def halves(chunk):
        h, first, count, at = chunk
        return pl.ds(first, count // 2), pl.ds(first + count // 2, count // 2)

    def gather_own(chunk, turn):
        h, _, _, at = chunk
        for way in (RIGHT, LEFT):
            block = xg.at[h, z, halves(chunk)[way ^ turn]]
            got = gr.at[at, 1 + way if turn else 0]
            send(block, block, gs.at[0], got, ctx, (z + STEP[way]) % N)

    def gather_relay(chunk):
        h, first, count, at = chunk
        arrive(xg.at[h, z, pl.ds(first, count)], gr.at[at, 0])
        for way in (RIGHT, LEFT):
            block = xg.at[h, (z + N - STEP[way]) % N, halves(chunk)[way]]
            send(block, block, gs.at[0], gr.at[at, 3], ctx, (z + STEP[way]) % N)

    def gather_rest(chunk, way):
        h, _, _, at = chunk
        arrive(xg.at[h, (z + N - STEP[way]) % N, halves(chunk)[1 - way]], gr.at[at, 1 + way])

    def gather_last(chunk):
        h, first, count, at = chunk
        arrive(xg.at[h, (z + 2) % N, pl.ds(first, count)], gr.at[at, 3])

    def weights(at):
        w_in[at].wait()

    def project_own():
        rows = pl.ds(pl.multiple_of(z * DW, DW), DW)

        def tile(j, carry):
            at = pl.ds(pl.multiple_of(j * DW, DW), DW)
            a = jnp.concatenate([xg[h, z] for h in range(2)], axis=0)
            part = jnp.dot(a, wq[j, rows, :], preferred_element_type=F32)
            for h in range(2):
                acc[h, :, at] = part[h * R : (h + 1) * R]
            return carry

        lax.fori_loop(0, 3, tile, 0)

    def project(chunk, rel):
        h, first, count, _ = chunk
        src = (z + rel) % N
        rows = pl.ds(pl.multiple_of(src * DW, DW), DW)
        mine = pl.ds(first, count)

        def tile(j, carry):
            at = pl.ds(pl.multiple_of(j * DW, DW), DW)
            acc[h, mine, at] += jnp.dot(
                xg[h, src, mine], wq[j, rows, :], preferred_element_type=F32
            )
            return carry

        lax.fori_loop(0, 3, tile, 0)

    def tables():
        perm_in.wait()
        tab_in.wait()
        for s in range(4):
            at = perm[4 * ctx + s]
            rows = pl.ds(s * WW, WW)
            cost[rows, :] = tab[pl.ds(at, 1), :] + tab[pl.ds(256, WW), :]
            sint[rows, :] = tab[pl.ds(128 + at, 1), :] + tab[pl.ds(256 + WW, WW), :]
        source = lax.broadcasted_iota(jnp.int32, (2 * HD, 2 * HD), 0)
        target = lax.broadcasted_iota(jnp.int32, (2 * HD, 2 * HD), 1)
        lane = target % HD
        distance = jnp.where(lane < 16, 8, 28)
        low = (lane < 8) | ((lane >= 16) & (lane < 44)) | ((lane >= 72) & (lane < 100))
        partner = target + jnp.where(low, distance, -distance)
        swap[...] = jnp.where(source == partner, 1.0, 0.0).astype(BF)

    def finish(chunk):
        h, first, count, _ = chunk
        mine = pl.ds(first, count)
        cosine = cost[pl.ds(h * R + first, count), :]
        sine = sint[pl.ds(h * R + first, count), :]
        for j in range(2):
            pairs = [acc[h, mine, pl.ds(j * DW + i * 2 * HD, 2 * HD)] for i in range(HH)]
            stacked = jnp.concatenate([p.astype(BF) for p in pairs], axis=0)
            other = jnp.dot(stacked, swap[...], preferred_element_type=F32)
            for head in range(2 * HH):
                cols = slice(head % 2 * HD, (head % 2 + 1) * HD)
                v = pairs[head // 2][:, cols]
                w = other[head // 2 * count : (head // 2 + 1) * count, cols]
                square = jnp.mean(v * v, axis=-1, keepdims=True)
                factor = lax.rsqrt(square + EPSILON)
                if j == 0:
                    factor = factor * (HD**-0.5 / math.log(2.0))
                turned = ((v * cosine + w * sine) * factor).astype(BF)
                half, to = head // HH, pl.ds(head % HH * HD, HD)
                if j == 0:
                    oq[half, h, mine, to] = turned
                else:
                    okv[half, h, 0, mine, to] = turned
        for half in range(2):
            okv[half, h, 1, mine] = acc[h, mine, pl.ds(2 * DW + half * HW, HW)].astype(BF)

    def spread(chunk):
        h, first, count, at = chunk
        rows = pl.ds(first, count)
        for turn in range(2):
            for half in range(2):
                qslot = (y, x)[half]
                for way in (RIGHT, LEFT):
                    part = halves(chunk)[way ^ turn]
                    src, dst = oq.at[half, h, part], qb.at[h, qslot, c, part]
                    send(src, dst, xs.at[0], xr.at[at, turn], q_to(half, STEP[way]), z)
        send(
            oq.at[1 - c, h, rows], qb.at[h, kc, c, rows], xs.at[2], xr.at[at, 2], sibling, z
        )
        qb[h, qc, c, rows] = oq[c, h, rows]
        for turn in range(2):
            for half in range(2):
                kslot = (x, y)[half]
                for way in (RIGHT, LEFT):
                    part = way ^ turn
                    src, dst = okv.at[half, h, part, rows], kv.at[h, kslot, c, part, rows]
                    send(src, dst, xs.at[0], xr.at[at, 4 + turn], kv_to(half, STEP[way]), z)
        send(
            okv.at[1 - c, h, :, rows], kv.at[h, qc, c, :, rows],
            xs.at[3], xr.at[at, 6], sibling, z,
        )
        kv[h, kc, c, :, rows] = okv[c, h, :, rows]

    def spread_relay_q(chunk):
        h, first, count, at = chunk
        arrive(qb.at[h, qc, :, pl.ds(first, count)], xr.at[at, 0])
        for way in (RIGHT, LEFT):
            for core in range(2):
                block = qb.at[h, (qc + N - STEP[way]) % N, core, halves(chunk)[way]]
                send(block, block, xs.at[1], xr.at[at, 3], my_q(STEP[way], c), z)

    def spread_relay_kv(chunk):
        h, first, count, at = chunk
        arrive(kv.at[h, kc, :, :, pl.ds(first, count)], xr.at[at, 4])
        for way in (RIGHT, LEFT):
            for core in range(2):
                block = kv.at[h, (kc + N - STEP[way]) % N, core, way, pl.ds(first, count)]
                send(block, block, xs.at[1], xr.at[at, 7], my_kv(STEP[way]), z)

    def spread_sibling_q(chunk):
        h, first, count, at = chunk
        arrive(qb.at[h, qc, 1 - c, pl.ds(first, count)], xr.at[at, 2])

    def spread_rest_q(chunk):
        h, first, count, at = chunk
        arrive(qb.at[h, qc, :, pl.ds(first, count)], xr.at[at, 1])

    def spread_rest_kv(chunk):
        h, first, count, at = chunk
        arrive(kv.at[h, kc, 1 - c, :, pl.ds(first, count)], xr.at[at, 6])
        arrive(kv.at[h, kc, :, :, pl.ds(first, count)], xr.at[at, 5])

    def spread_last_q(chunk):
        h, first, count, at = chunk
        arrive(qb.at[h, (qc + 2) % N, :, pl.ds(first, count)], xr.at[at, 3])

    def spread_last_kv(chunk):
        h, first, count, at = chunk
        arrive(kv.at[h, (kc + 2) % N, :, :, pl.ds(first, count)], xr.at[at, 7])

    frame_rows = perm.shape[0] // 8

    def attend(queries, against):
        rows = [(h, (qc + rel) % N, a, first) for h, rel, first in queries for a in range(2)]
        keys = [(h, (kc + rel) % N, b) for h, rel in against for b in range(2)]
        fq = [
            perm[4 * cid((1 - c) * t + c * y, (1 - c) * x + c * t, a) + 2 * h] // frame_rows
            for h, t, a, _ in rows
        ]
        fk = [
            perm[4 * cid((1 - c) * y + c * t, (1 - c) * t + c * x, b) + 2 * h] // frame_rows
            for h, t, b in keys
        ]

        def seen(w, n, m):
            block = w[n * R : (n + 1) * R, m * R : (m + 1) * R]
            return block * (fk[m] <= fq[n]).astype(F32) if rows[n][0] == keys[m][0] else block

        for i in range(HH):
            cols = pl.ds(i * HD, HD)
            q = jnp.concatenate([qb[h, t, a, :, cols] for h, t, a, _ in rows], axis=0)
            k = jnp.concatenate([kv[h, t, b, 0, :, cols] for h, t, b in keys], axis=0)
            v = jnp.concatenate([kv[h, t, b, 1, :, cols] for h, t, b in keys], axis=0)
            s = lax.dot_general(q, k, (((1,), (1,)), ((), ())), preferred_element_type=F32)
            w = jnp.exp2(s)
            w = jnp.concatenate(
                [
                    jnp.concatenate([seen(w, n, m) for m in range(len(keys))], axis=1)
                    for n in range(len(rows))
                ],
                axis=0,
            )
            total = w[:, :HD]
            for b in range(1, len(keys)):
                total = total + w[:, b * HD : (b + 1) * HD]
            o = jnp.dot(w.astype(BF), v, preferred_element_type=F32)
            for n, (h, t, a, first) in enumerate(rows):
                piece = slice(n * R, (n + 1) * R)
                if first:
                    num[h, t, a, :, cols] = o[piece]
                    den[h, t, a, :, cols] = total[piece]
                else:
                    num[h, t, a, :, cols] += o[piece]
                    den[h, t, a, :, cols] += total[piece]

    def row_sum(h, slot, core, i):
        return jnp.sum(den[h, slot, core, :, pl.ds(i * HD, HD)].T, axis=0, keepdims=True)

    def pack(dst, h, slot, core, plus=None):
        for i in range(HH):
            cols = pl.ds(i * HD, HD)
            n = num[h, slot, core, :, cols]
            d = row_sum(h, slot, core, i)
            if plus is not None:
                n = n + plus[pl.ds(0, R), cols].astype(F32)
                d = d + plus[pl.ds(R, 8), cols].astype(F32)
            dst[pl.ds(0, R), cols] = n.astype(BF)
            dst[pl.ds(R, 8), cols] = jnp.broadcast_to(d, (8, HD)).astype(BF)

    def sum_far(h):
        far = (qc + 2) % N
        for way in (RIGHT, LEFT):
            pack(os1.at[h, way], h, far, way)
            send(os1.at[h, way], or1.at[h, way], o1s.at[0], o1r.at[h], my_q(STEP[way], c), z)

    def near_pack(h, way, core, plus=None):
        pack(os2.at[h, way, core], h, (qc + STEP[way]) % N, core, plus)

    def near_send(h, way, core):
        src, dst = os2.at[h, way, core], or2.at[h, c, way]
        send(src, dst, o2s.at[0], o2r.at[h], my_q(STEP[way], core), z)

    def sum_plain(h, way):
        near_pack(h, way, 1 - way)
        near_send(h, way, 1 - way)

    def sum_passed(h):
        arrive(or1.at[h], o1r.at[h])
        for way in (RIGHT, LEFT):
            near_pack(h, way, way, or1.at[h, way])
            near_send(h, way, way)

    def sum_sibling(h):
        pack(oss.at[h], h, qc, 1 - c)
        send(oss.at[h], ors.at[h], oqs.at[0], oqr.at[h], sibling, z)

    def normalize(h):
        arrive(or2.at[h], o2r.at[h])
        arrive(ors.at[h], oqr.at[h])
        for mine in range(2):
            half = c if mine else 1 - c
            for i in range(HH):
                cols = pl.ds(i * HD, HD)
                if mine:
                    n = num[h, qc, c, :, cols]
                    d = row_sum(h, qc, c, i)
                else:
                    n = ors[h, pl.ds(0, R), cols].astype(F32)
                    d = ors[h, pl.ds(R, 8), cols].astype(F32)[:1]
                for way in (RIGHT, LEFT):
                    n = n + or2[h, half, way, pl.ds(0, R), cols].astype(F32)
                    d = d + or2[h, half, way, pl.ds(R, 8), cols].astype(F32)[:1]
                attn[h, half, :, cols] = (n / jnp.broadcast_to(d, (HD, R)).T).astype(BF)

    def mixed_for(h, rel, store):
        base = (z + rel) % N * DW

        for t in range(3):
            cols = pl.ds(pl.multiple_of(base + t * 256, 256), 256)
            part = jnp.dot(attn[h, 0], wo[pl.ds(0, HW), cols], preferred_element_type=F32)
            part += jnp.dot(attn[h, 1], wo[pl.ds(HW, HW), cols], preferred_element_type=F32)
            store(pl.ds(t * 256, 256), part)

    def mix_far(h):
        def store(cols, part):
            for way in (RIGHT, LEFT):
                zs1[h, way, :, cols] = part[way * (R // 2) : (way + 1) * (R // 2)].astype(BF)

        mixed_for(h, 2, store)
        for way in (RIGHT, LEFT):
            send(zs1.at[h, way], zr1.at[h, way], z1s.at[0], z1r.at[h], ctx, (z + STEP[way]) % N)

    def mix_send(h, way, part):
        src, dst = zs2.at[h, way, part], zr2.at[h, way, part]
        send(src, dst, z2s.at[0], z2r.at[h], ctx, (z + STEP[way]) % N)

    def mix_plain(h, way):
        part = 1 - way

        def store(cols, rows):
            zp[h, way, :, cols] = rows[way * (R // 2) : (way + 1) * (R // 2)]
            zs2[h, way, part, :, cols] = rows[part * (R // 2) : (part + 1) * (R // 2)].astype(BF)

        mixed_for(h, STEP[way], store)
        mix_send(h, way, part)

    def mix_own(h):
        def store(cols, rows):
            own[h, :, cols] = rows

        mixed_for(h, 0, store)

    def mix_passed(h):
        arrive(zr1.at[h], z1r.at[h])
        for way in (RIGHT, LEFT):
            zs2[h, way, way] = (zp[h, way] + zr1[h, way].astype(F32)).astype(BF)
            mix_send(h, way, way)

    def mix_last(h):
        arrive(zr2.at[h], z2r.at[h])
        for part in range(2):
            total = own[h, half_rows[part], :]
            for way in (RIGHT, LEFT):
                total = total + zr2[h, way, part].astype(F32)
            mixed[h, half_rows[part], :] = total.astype(BF)
        copy = pltpu.make_async_copy(mixed.at[h], out.at[pl.ds(h * R, R)], lsem.at[h])
        copy.start()
        outgoing.append(copy)

    near = (1, 3, 0)
    early = [(EARLY, rel) for rel in (1, 3, 0, 2)]
    late = [(LATE, rel) for rel in (1, 3, 0, 2)]
    outgoing = []
    tok_in[0].wait()
    gather_own(C0, 0)
    gather_own(C0, 1)
    gather_own(C1, 0)
    tables()
    tok_in[1].wait()
    weights(0)
    project_own()
    gather_relay(C0)
    gather_own(C1, 1)
    weights(1)
    gather_rest(C0, RIGHT)
    project(C0, 3)
    gather_relay(C1)
    gather_own(C2, 0)
    gather_own(C2, 1)
    weights(2)
    gather_rest(C0, LEFT)
    project(C0, 1)
    weights(3)
    gather_last(C0)
    project(C0, 2)
    finish(C0)
    spread(C0)
    gather_rest(C1, RIGHT)
    project(C1, 3)
    gather_rest(C1, LEFT)
    project(C1, 1)
    gather_last(C1)
    project(C1, 2)
    gather_relay(C2)
    finish(C1)
    spread(C1)
    gather_rest(C2, RIGHT)
    project(C2, 3)
    spread_relay_q(C0)
    spread_relay_kv(C0)
    gather_rest(C2, LEFT)
    project(C2, 1)
    gather_last(C2)
    spread_relay_q(C1)
    spread_relay_kv(C1)
    project(C2, 2)
    finish(C2)
    spread(C2)
    spread_sibling_q(C0)
    spread_sibling_q(C1)
    spread_rest_q(C0)
    spread_rest_q(C1)
    spread_rest_kv(C0)
    spread_rest_kv(C1)
    attend([(EARLY, rel, True) for rel in near], early[:3])
    spread_sibling_q(C2)
    attend([(LATE, 0, True)], early[:3])
    spread_last_q(C0)
    spread_last_q(C1)
    spread_last_kv(C0)
    spread_last_kv(C1)
    attend([(EARLY, 2, True)], early)
    spread_relay_q(C2)
    sum_far(0)
    attend([(EARLY, rel, False) for rel in near] + [(LATE, 0, False)], early[3:])
    spread_rest_q(C2)
    attend([(LATE, 1, True)], early)
    spread_relay_kv(C2)
    attend([(LATE, 3, True)], early)
    near_pack(0, RIGHT, LEFT)
    near_pack(0, LEFT, RIGHT)
    sum_sibling(0)
    spread_rest_kv(C2)
    attend([(LATE, rel, False) for rel in near], late[:3])
    near_send(0, RIGHT, LEFT)
    near_send(0, LEFT, RIGHT)
    spread_last_q(C2)
    attend([(LATE, 2, True)], early + late[:3])
    sum_passed(0)
    spread_last_kv(C2)
    attend([(LATE, 2, False)], late[3:])
    sum_far(1)
    attend([(LATE, rel, False) for rel in near], late[3:])
    sum_plain(1, RIGHT)
    sum_plain(1, LEFT)
    sum_sibling(1)
    wo_in.wait()
    normalize(0)
    mix_far(0)
    sum_passed(1)
    mix_plain(0, RIGHT)
    mix_plain(0, LEFT)
    mix_own(0)
    mix_passed(0)
    normalize(1)
    mix_far(1)
    mix_plain(1, RIGHT)
    mix_plain(1, LEFT)
    mix_own(1)
    mix_last(0)
    mix_passed(1)
    mix_last(1)
    left_here(xg.at[:, pl.ds(0, 3)], gs.at[0])
    left_here(kv.at[:, pl.ds(0, 3)], xs.at[0])
    left_here(qb.at[:, pl.ds(0, 3)], xs.at[1])
    left_here(oq.at[1 - c], xs.at[2])
    left_here(okv.at[1 - c], xs.at[3])
    left_here(os1, o1s.at[0])
    left_here(os2, o2s.at[0])
    left_here(oss, oqs.at[0])
    left_here(zs1, z1s.at[0])
    left_here(zs2, z2s.at[0])
    for copy in outgoing:
        copy.wait()


def per_device(tokens, w_qkv, w_out, block_perm):
    table = jnp.asarray(np.concatenate(rope_tables(block_perm.shape[0] // 8)))
    hbm = pl.BlockSpec(memory_space=pl.ANY)
    dma = pltpu.SemaphoreType.DMA
    return pl.pallas_call(
        kernel,
        name="attention_layer",
        out_shape=jax.ShapeDtypeStruct((2 * R, DW), BF),
        in_specs=[hbm] * 5,
        out_specs=hbm,
        scratch_shapes=[
            pltpu.SMEM(block_perm.shape, jnp.int32),
            pltpu.VMEM(table.shape, F32),
            pltpu.VMEM((2, N, R, DW), BF),
            pltpu.VMEM((3, N * DW, DW), BF),
            pltpu.VMEM((DW, N * DW), BF),
            pltpu.VMEM((2, R, 3 * DW), F32),
            pltpu.VMEM((2 * R, HD), F32),
            pltpu.VMEM((2 * R, HD), F32),
            pltpu.VMEM((2 * HD, 2 * HD), BF),
            pltpu.VMEM((2, 2, 2, R, HW), BF),
            pltpu.VMEM((2, 2, R, HW), BF),
            pltpu.VMEM((2, N, 2, 2, R, HW), BF),
            pltpu.VMEM((2, N, 2, R, HW), BF),
            pltpu.VMEM((2, N, 2, R, HW), F32),
            pltpu.VMEM((2, N, 2, R, HW), F32),
            pltpu.VMEM((2, 2, OB, HW), BF),
            pltpu.VMEM((2, 2, OB, HW), BF),
            pltpu.VMEM((2, 2, 2, OB, HW), BF),
            pltpu.VMEM((2, 2, 2, OB, HW), BF),
            pltpu.VMEM((2, OB, HW), BF),
            pltpu.VMEM((2, OB, HW), BF),
            pltpu.VMEM((2, 2, R, HW), BF),
            pltpu.VMEM((2, 2, R // 2, DW), BF),
            pltpu.VMEM((2, 2, R // 2, DW), BF),
            pltpu.VMEM((2, 2, R // 2, DW), F32),
            pltpu.VMEM((2, R, DW), F32),
            pltpu.VMEM((2, 2, 2, R // 2, DW), BF),
            pltpu.VMEM((2, 2, 2, R // 2, DW), BF),
            pltpu.VMEM((2, R, DW), BF),
            dma((9,)),
            dma((1,)),
            dma((3, 4)),
            dma((4,)),
            dma((3, 8)),
            dma((1,)),
            dma((2,)),
            dma((1,)),
            dma((2,)),
            dma((1,)),
            dma((2,)),
            dma((1,)),
            dma((2,)),
            dma((1,)),
            dma((2,)),
        ],
        compiler_params=pltpu.CompilerParams(
            collective_id=0, has_side_effects=True, vmem_limit_bytes=64 * 1024 * 1024 - 65536
        ),
    )(block_perm, table, tokens, w_qkv, w_out)


def solution(mesh):
    in_specs = (P("ctx", "head"), P(None, None, "head"), P("head", None), P())
    return jax.shard_map(
        per_device, mesh=mesh, in_specs=in_specs, out_specs=P("ctx", "head"), check_vma=False
    )
```

```python
import functools
import math

import jax
import jax.numpy as jnp
import numpy as np
from jax import lax
from jax.experimental import pallas as pl
from jax.experimental.pallas import tpu as pltpu
from jax.sharding import PartitionSpec as P

HD = 128
WW = 64
ROPE_BASE = 10000.0
EPSILON = 1e-06
N = 4
R = 128
HH = 3
HW = HH * HD
DW = 2 * HW
OB = R + 8
BF = jnp.bfloat16
F32 = jnp.float32
RIGHT, LEFT = 0, 1
EARLY, LATE = 0, 1
C0, C1, C2 = (EARLY, 0, R // 2, 0), (EARLY, R // 2, R // 2, 1), (LATE, 0, R, 2)
STEP = (1, N - 1)


def rope_tables(frame_rows):
    parts = ((0, HD // 16), (HD // 8, 7 * HD // 32), (HD // 8 + 7 * HD // 16, 7 * HD // 32))
    frames = np.arange(128) // frame_rows
    rows = np.arange(128) % frame_rows
    tables = []
    for position, kinds in ((np.stack([frames, rows]), (0, 1)), (np.arange(WW)[None], (2,))):
        cosine = np.zeros((position.shape[1], HD), np.float32)
        sine = np.zeros((position.shape[1], HD), np.float32)
        for at, kind in enumerate(kinds):
            first, pairs = parts[kind]
            freq = np.float32(ROPE_BASE) ** (-np.arange(pairs, dtype=np.float32) / pairs)
            angle = position[at].astype(np.float32)[:, None] * freq[None, :].astype(np.float32)
            cosine[:, first : first + pairs] = np.cos(angle)
            cosine[:, first + pairs : first + 2 * pairs] = np.cos(angle)
            sine[:, first : first + pairs] = -np.sin(angle)
            sine[:, first + pairs : first + 2 * pairs] = np.sin(angle)
        tables += [cosine, sine]
    return tables


def kernel(
    perm_hbm, tab_hbm, tok, wqkv, wout, out,
    perm, tab, xg, wq, wo, acc, cost, sint, swap, okv, oq, kv, qb, num, den,
    os1, or1, os2, or2, oss, ors, attn, zs1, zr1, zp, own, zs2, zr2, mixed,
    lsem, gs, gr, xs, xr, o1s, o1r, o2s, o2r, oqs, oqr, z1s, z1r, z2s, z2r,
):
    ctx = lax.axis_index("ctx")
    z = lax.axis_index("head")
    c = ctx % 2
    x = (ctx // 2) % N
    y = ctx // (2 * N)

    def cid(yy, xx, cc):
        return (yy * N + xx) * 2 + cc

    def kv_to(half, d):
        if half == 0:
            return cid(y, (x + d) % N, 0)
        return cid((y + d) % N, x, 1)

    def q_to(half, d):
        if half == 0:
            return cid((y + d) % N, x, 0)
        return cid(y, (x + d) % N, 1)

    def my_kv(d):
        return cid((y + c * d) % N, (x + (1 - c) * d) % N, c)

    def my_q(d, core):
        return cid((y + (1 - c) * d) % N, (x + c * d) % N, core)

    sibling = cid(y, x, 1 - c)
    kc = x * (1 - c) + y * c
    qc = y * (1 - c) + x * c

    def send(src, dst, ss, rs, to_ctx, to_z):
        pltpu.make_async_remote_copy(
            src_ref=src, dst_ref=dst, send_sem=ss, recv_sem=rs,
            device_id=(to_ctx, to_z), device_id_type=pl.DeviceIdType.MESH,
        ).start()

    def sized(ref, sem):
        return pltpu.make_async_remote_copy(
            src_ref=ref, dst_ref=ref, send_sem=sem, recv_sem=sem,
            device_id=(sibling, z), device_id_type=pl.DeviceIdType.MESH,
        )

    def arrive(dst, rs):
        sized(dst, rs).wait_recv()

    def left_here(src, ss):
        sized(src, ss).wait_send()

    perm_in = pltpu.make_async_copy(perm_hbm, perm, lsem.at[7])
    perm_in.start()
    tab_in = pltpu.make_async_copy(tab_hbm, tab, lsem.at[8])
    tab_in.start()
    tok_in = [
        pltpu.make_async_copy(tok.at[pl.ds(h * R, R)], xg.at[h, z], lsem.at[h]) for h in range(2)
    ]
    for copy in tok_in:
        copy.start()
    w_in = []
    for at, rel in enumerate((0, 3, 1, 2)):
        rows = pl.ds(pl.multiple_of((z + rel) % N * DW, DW), DW)
        w_in.append(pltpu.make_async_copy(wqkv.at[:, rows], wq.at[:, rows], lsem.at[2 + at]))
    for copy in w_in:
        copy.start()
    wo_in = pltpu.make_async_copy(wout, wo, lsem.at[6])
    wo_in.start()

    barrier = pltpu.get_barrier_semaphore()
    peers = [(sibling, z)]
    for d in STEP:
        peers.append((ctx, (z + d) % N))
        for core in range(2):
            peers.append((cid(y, (x + d) % N, core), z))
            peers.append((cid((y + d) % N, x, core), z))
    for peer in peers:
        pl.semaphore_signal(barrier, inc=1, device_id=peer, device_id_type=pl.DeviceIdType.MESH)
    pl.semaphore_wait(barrier, len(peers))

    half_rows = (pl.ds(0, R // 2), pl.ds(R // 2, R // 2))

    def halves(chunk):
        h, first, count, at = chunk
        return pl.ds(first, count // 2), pl.ds(first + count // 2, count // 2)

    def gather_own(chunk, turn):
        h, _, _, at = chunk
        for way in (RIGHT, LEFT):
            block = xg.at[h, z, halves(chunk)[way ^ turn]]
            got = gr.at[at, 1 + way if turn else 0]
            send(block, block, gs.at[0], got, ctx, (z + STEP[way]) % N)

    def gather_relay(chunk):
        h, first, count, at = chunk
        arrive(xg.at[h, z, pl.ds(first, count)], gr.at[at, 0])
        for way in (RIGHT, LEFT):
            block = xg.at[h, (z + N - STEP[way]) % N, halves(chunk)[way]]
            send(block, block, gs.at[0], gr.at[at, 3], ctx, (z + STEP[way]) % N)

    def gather_rest(chunk, way):
        h, _, _, at = chunk
        arrive(xg.at[h, (z + N - STEP[way]) % N, halves(chunk)[1 - way]], gr.at[at, 1 + way])

    def gather_last(chunk):
        h, first, count, at = chunk
        arrive(xg.at[h, (z + 2) % N, pl.ds(first, count)], gr.at[at, 3])

    def weights(at):
        w_in[at].wait()

    def project_own():
        rows = pl.ds(pl.multiple_of(z * DW, DW), DW)

        def tile(j, carry):
            at = pl.ds(pl.multiple_of(j * DW, DW), DW)
            a = jnp.concatenate([xg[h, z] for h in range(2)], axis=0)
            part = jnp.dot(a, wq[j, rows, :], preferred_element_type=F32)
            for h in range(2):
                acc[h, :, at] = part[h * R : (h + 1) * R]
            return carry

        lax.fori_loop(0, 3, tile, 0)

    def project(chunk, rel):
        h, first, count, _ = chunk
        src = (z + rel) % N
        rows = pl.ds(pl.multiple_of(src * DW, DW), DW)
        mine = pl.ds(first, count)

        def tile(j, carry):
            at = pl.ds(pl.multiple_of(j * DW, DW), DW)
            acc[h, mine, at] += jnp.dot(
                xg[h, src, mine], wq[j, rows, :], preferred_element_type=F32
            )
            return carry

        lax.fori_loop(0, 3, tile, 0)

    def tables():
        perm_in.wait()
        tab_in.wait()
        for s in range(4):
            at = perm[4 * ctx + s]
            rows = pl.ds(s * WW, WW)
            cost[rows, :] = tab[pl.ds(at, 1), :] + tab[pl.ds(256, WW), :]
            sint[rows, :] = tab[pl.ds(128 + at, 1), :] + tab[pl.ds(256 + WW, WW), :]
        source = lax.broadcasted_iota(jnp.int32, (2 * HD, 2 * HD), 0)
        target = lax.broadcasted_iota(jnp.int32, (2 * HD, 2 * HD), 1)
        lane = target % HD
        distance = jnp.where(lane < 16, 8, 28)
        low = (lane < 8) | ((lane >= 16) & (lane < 44)) | ((lane >= 72) & (lane < 100))
        partner = target + jnp.where(low, distance, -distance)
        swap[...] = jnp.where(source == partner, 1.0, 0.0).astype(BF)

    def finish(chunk, j):
        h, first, count, _ = chunk
        mine = pl.ds(first, count)
        cosine = cost[pl.ds(h * R + first, count), :]
        sine = sint[pl.ds(h * R + first, count), :]
        if j == 2:
            for half in range(2):
                okv[half, h, 1, mine] = acc[h, mine, pl.ds(2 * DW + half * HW, HW)].astype(BF)
            return
        pairs = [acc[h, mine, pl.ds(j * DW + i * 2 * HD, 2 * HD)] for i in range(HH)]
        stacked = jnp.concatenate([p.astype(BF) for p in pairs], axis=0)
        other = jnp.dot(stacked, swap[...], preferred_element_type=F32)
        for head in range(2 * HH):
            cols = slice(head % 2 * HD, (head % 2 + 1) * HD)
            v = pairs[head // 2][:, cols]
            w = other[head // 2 * count : (head // 2 + 1) * count, cols]
            square = jnp.mean(v * v, axis=-1, keepdims=True)
            factor = lax.rsqrt(square + EPSILON)
            if j == 0:
                factor = factor * (HD**-0.5 / math.log(2.0))
            turned = ((v * cosine + w * sine) * factor).astype(BF)
            half, to = head // HH, pl.ds(head % HH * HD, HD)
            if j == 0:
                oq[half, h, mine, to] = turned
            else:
                okv[half, h, 0, mine, to] = turned

    def project_last(chunk):
        h, first, count, _ = chunk
        src = (z + 2) % N
        rows = pl.ds(pl.multiple_of(src * DW, DW), DW)
        mine = pl.ds(first, count)
        for j in range(3):
            acc[h, mine, pl.ds(j * DW, DW)] += jnp.dot(
                xg[h, src, mine], wq[j, rows, :], preferred_element_type=F32
            )
            finish(chunk, j)
            if j == 0:
                spread_q(chunk)
            else:
                spread_kv(chunk, j - 1)

    def spread_q(chunk):
        h, first, count, at = chunk
        rows = pl.ds(first, count)
        for turn in range(2):
            for half in range(2):
                qslot = (y, x)[half]
                for way in (RIGHT, LEFT):
                    part = halves(chunk)[way ^ turn]
                    src, dst = oq.at[half, h, part], qb.at[h, qslot, c, part]
                    send(src, dst, xs.at[0], xr.at[at, turn], q_to(half, STEP[way]), z)
        send(
            oq.at[1 - c, h, rows], qb.at[h, kc, c, rows], xs.at[2], xr.at[at, 2], sibling, z
        )
        qb[h, qc, c, rows] = oq[c, h, rows]

    def spread_kv(chunk, part):
        h, first, count, at = chunk
        rows = pl.ds(first, count)
        for half in range(2):
            kslot = (x, y)[half]
            for way in (RIGHT, LEFT):
                src, dst = okv.at[half, h, part, rows], kv.at[h, kslot, c, part, rows]
                send(src, dst, xs.at[0], xr.at[at, 4 + part], kv_to(half, STEP[way]), z)
        if part == 1:
            send(
                okv.at[1 - c, h, :, rows], kv.at[h, qc, c, :, rows],
                xs.at[3], xr.at[at, 6], sibling, z,
            )
            kv[h, kc, c, :, rows] = okv[c, h, :, rows]

    def spread_relay_q(chunk):
        h, first, count, at = chunk
        arrive(qb.at[h, qc, :, pl.ds(first, count)], xr.at[at, 0])
        for way in (RIGHT, LEFT):
            for core in range(2):
                block = qb.at[h, (qc + N - STEP[way]) % N, core, halves(chunk)[way]]
                send(block, block, xs.at[1], xr.at[at, 3], my_q(STEP[way], c), z)

    def spread_relay_kv(chunk, part):
        h, first, count, at = chunk
        rows = pl.ds(first, count)
        arrive(kv.at[h, kc, :, :, rows], xr.at[at, 4 + part])
        for way in (RIGHT, LEFT):
            block = kv.at[h, (kc + N - STEP[way]) % N, way, part, rows]
            send(block, block, xs.at[1], xr.at[at, 7], my_kv(STEP[way]), z)

    def spread_sibling_q(chunk):
        h, first, count, at = chunk
        arrive(qb.at[h, qc, 1 - c, pl.ds(first, count)], xr.at[at, 2])

    def spread_rest_q(chunk):
        h, first, count, at = chunk
        arrive(qb.at[h, qc, :, pl.ds(first, count)], xr.at[at, 1])

    def spread_rest_kv(chunk):
        h, first, count, at = chunk
        arrive(kv.at[h, kc, 1 - c, :, pl.ds(first, count)], xr.at[at, 6])

    def spread_last_q(chunk):
        h, first, count, at = chunk
        arrive(qb.at[h, (qc + 2) % N, :, pl.ds(first, count)], xr.at[at, 3])

    def spread_last_kv(chunk):
        h, first, count, at = chunk
        arrive(kv.at[h, (kc + 2) % N, :, :, pl.ds(first, count)], xr.at[at, 7])

    frame_rows = perm.shape[0] // 8

    def attend(queries, against):
        rows = [(h, (qc + rel) % N, a, first) for h, rel, first in queries for a in range(2)]
        keys = [(h, (kc + rel) % N, b) for h, rel in against for b in range(2)]
        fq = [
            perm[4 * cid((1 - c) * t + c * y, (1 - c) * x + c * t, a) + 2 * h] // frame_rows
            for h, t, a, _ in rows
        ]
        fk = [
            perm[4 * cid((1 - c) * y + c * t, (1 - c) * t + c * x, b) + 2 * h] // frame_rows
            for h, t, b in keys
        ]

        def seen(w, n, m):
            block = w[n * R : (n + 1) * R, m * R : (m + 1) * R]
            return block * (fk[m] <= fq[n]).astype(F32) if rows[n][0] == keys[m][0] else block

        for i in range(HH):
            cols = pl.ds(i * HD, HD)
            q = jnp.concatenate([qb[h, t, a, :, cols] for h, t, a, _ in rows], axis=0)
            k = jnp.concatenate([kv[h, t, b, 0, :, cols] for h, t, b in keys], axis=0)
            v = jnp.concatenate([kv[h, t, b, 1, :, cols] for h, t, b in keys], axis=0)
            s = lax.dot_general(q, k, (((1,), (1,)), ((), ())), preferred_element_type=F32)
            w = jnp.exp2(s)
            w = jnp.concatenate(
                [
                    jnp.concatenate([seen(w, n, m) for m in range(len(keys))], axis=1)
                    for n in range(len(rows))
                ],
                axis=0,
            )
            total = w[:, :HD]
            for b in range(1, len(keys)):
                total = total + w[:, b * HD : (b + 1) * HD]
            o = jnp.dot(w.astype(BF), v, preferred_element_type=F32)
            for n, (h, t, a, first) in enumerate(rows):
                piece = slice(n * R, (n + 1) * R)
                if first:
                    num[h, t, a, :, cols] = o[piece]
                    den[h, t, a, :, cols] = total[piece]
                else:
                    num[h, t, a, :, cols] += o[piece]
                    den[h, t, a, :, cols] += total[piece]

    def row_sum(h, slot, core, i):
        return jnp.sum(den[h, slot, core, :, pl.ds(i * HD, HD)].T, axis=0, keepdims=True)

    def pack(dst, h, slot, core, plus=None):
        for i in range(HH):
            cols = pl.ds(i * HD, HD)
            n = num[h, slot, core, :, cols]
            d = row_sum(h, slot, core, i)
            if plus is not None:
                n = n + plus[pl.ds(0, R), cols].astype(F32)
                d = d + plus[pl.ds(R, 8), cols].astype(F32)
            dst[pl.ds(0, R), cols] = n.astype(BF)
            dst[pl.ds(R, 8), cols] = jnp.broadcast_to(d, (8, HD)).astype(BF)

    def sum_far(h):
        far = (qc + 2) % N
        for way in (RIGHT, LEFT):
            pack(os1.at[h, way], h, far, way)
            send(os1.at[h, way], or1.at[h, way], o1s.at[0], o1r.at[h], my_q(STEP[way], c), z)

    def near_pack(h, way, core, plus=None):
        pack(os2.at[h, way, core], h, (qc + STEP[way]) % N, core, plus)

    def near_send(h, way, core):
        src, dst = os2.at[h, way, core], or2.at[h, c, way]
        send(src, dst, o2s.at[0], o2r.at[h], my_q(STEP[way], core), z)

    def sum_plain(h, way):
        near_pack(h, way, 1 - way)
        near_send(h, way, 1 - way)

    def sum_passed(h):
        arrive(or1.at[h], o1r.at[h])
        for way in (RIGHT, LEFT):
            near_pack(h, way, way, or1.at[h, way])
            near_send(h, way, way)

    def sum_sibling(h):
        pack(oss.at[h], h, qc, 1 - c)
        send(oss.at[h], ors.at[h], oqs.at[0], oqr.at[h], sibling, z)

    def normalize(h):
        arrive(or2.at[h], o2r.at[h])
        arrive(ors.at[h], oqr.at[h])
        for mine in range(2):
            half = c if mine else 1 - c
            for i in range(HH):
                cols = pl.ds(i * HD, HD)
                if mine:
                    n = num[h, qc, c, :, cols]
                    d = row_sum(h, qc, c, i)
                else:
                    n = ors[h, pl.ds(0, R), cols].astype(F32)
                    d = ors[h, pl.ds(R, 8), cols].astype(F32)[:1]
                for way in (RIGHT, LEFT):
                    n = n + or2[h, half, way, pl.ds(0, R), cols].astype(F32)
                    d = d + or2[h, half, way, pl.ds(R, 8), cols].astype(F32)[:1]
                attn[h, half, :, cols] = (n / jnp.broadcast_to(d, (HD, R)).T).astype(BF)

    def mixed_for(h, rel, store):
        base = (z + rel) % N * DW

        for t in range(3):
            cols = pl.ds(pl.multiple_of(base + t * 256, 256), 256)
            part = jnp.dot(attn[h, 0], wo[pl.ds(0, HW), cols], preferred_element_type=F32)
            part += jnp.dot(attn[h, 1], wo[pl.ds(HW, HW), cols], preferred_element_type=F32)
            store(pl.ds(t * 256, 256), part)

    def mix_far(h):
        def store(cols, part):
            for way in (RIGHT, LEFT):
                zs1[h, way, :, cols] = part[way * (R // 2) : (way + 1) * (R // 2)].astype(BF)

        mixed_for(h, 2, store)
        for way in (RIGHT, LEFT):
            send(zs1.at[h, way], zr1.at[h, way], z1s.at[0], z1r.at[h], ctx, (z + STEP[way]) % N)

    def mix_send(h, way, part):
        src, dst = zs2.at[h, way, part], zr2.at[h, way, part]
        send(src, dst, z2s.at[0], z2r.at[h], ctx, (z + STEP[way]) % N)

    def mix_plain(h, way):
        part = 1 - way

        def store(cols, rows):
            zp[h, way, :, cols] = rows[way * (R // 2) : (way + 1) * (R // 2)]
            zs2[h, way, part, :, cols] = rows[part * (R // 2) : (part + 1) * (R // 2)].astype(BF)

        mixed_for(h, STEP[way], store)
        mix_send(h, way, part)

    def mix_own(h):
        def store(cols, rows):
            own[h, :, cols] = rows

        mixed_for(h, 0, store)

    def mix_passed(h):
        arrive(zr1.at[h], z1r.at[h])
        for way in (RIGHT, LEFT):
            zs2[h, way, way] = (zp[h, way] + zr1[h, way].astype(F32)).astype(BF)
            mix_send(h, way, way)

    def mix_last(h):
        arrive(zr2.at[h], z2r.at[h])
        for part in range(2):
            total = own[h, half_rows[part], :]
            for way in (RIGHT, LEFT):
                total = total + zr2[h, way, part].astype(F32)
            mixed[h, half_rows[part], :] = total.astype(BF)
        copy = pltpu.make_async_copy(mixed.at[h], out.at[pl.ds(h * R, R)], lsem.at[h])
        copy.start()
        outgoing.append(copy)

    near = (1, 3, 0)
    early = [(EARLY, rel) for rel in (1, 3, 0, 2)]
    late = [(LATE, rel) for rel in (1, 3, 0, 2)]
    outgoing = []
    tok_in[0].wait()
    gather_own(C0, 0)
    gather_own(C0, 1)
    gather_own(C1, 0)
    tables()
    tok_in[1].wait()
    weights(0)
    project_own()
    gather_relay(C0)
    gather_own(C1, 1)
    weights(1)
    gather_rest(C0, RIGHT)
    project(C0, 3)
    gather_relay(C1)
    gather_own(C2, 0)
    gather_own(C2, 1)
    weights(2)
    gather_rest(C0, LEFT)
    project(C0, 1)
    weights(3)
    gather_last(C0)
    project_last(C0)
    gather_rest(C1, RIGHT)
    project(C1, 3)
    gather_rest(C1, LEFT)
    project(C1, 1)
    gather_last(C1)
    project_last(C1)
    gather_relay(C2)
    gather_rest(C2, RIGHT)
    project(C2, 3)
    spread_relay_q(C0)
    spread_relay_kv(C0, 0)
    gather_rest(C2, LEFT)
    project(C2, 1)
    spread_relay_kv(C0, 1)
    gather_last(C2)
    spread_relay_q(C1)
    spread_relay_kv(C1, 0)
    project_last(C2)
    spread_relay_kv(C1, 1)
    spread_sibling_q(C0)
    spread_sibling_q(C1)
    spread_rest_q(C0)
    spread_rest_q(C1)
    spread_rest_kv(C0)
    spread_rest_kv(C1)
    attend([(EARLY, rel, True) for rel in near], early[:3])
    spread_sibling_q(C2)
    attend([(LATE, 0, True)], early[:3])
    spread_last_q(C0)
    spread_last_q(C1)
    spread_last_kv(C0)
    spread_last_kv(C1)
    attend([(EARLY, 2, True)], early)
    spread_relay_q(C2)
    sum_far(0)
    attend([(EARLY, rel, False) for rel in near] + [(LATE, 0, False)], early[3:])
    spread_rest_q(C2)
    attend([(LATE, 1, True)], early)
    spread_relay_kv(C2, 0)
    attend([(LATE, 3, True)], early)
    near_pack(0, RIGHT, LEFT)
    near_pack(0, LEFT, RIGHT)
    sum_sibling(0)
    spread_rest_kv(C2)
    spread_relay_kv(C2, 1)
    attend([(LATE, rel, False) for rel in near], late[:3])
    near_send(0, RIGHT, LEFT)
    near_send(0, LEFT, RIGHT)
    spread_last_q(C2)
    attend([(LATE, 2, True)], early + late[:3])
    sum_passed(0)
    spread_last_kv(C2)
    attend([(LATE, 2, False)], late[3:])
    sum_far(1)
    attend([(LATE, rel, False) for rel in near], late[3:])
    sum_plain(1, RIGHT)
    sum_plain(1, LEFT)
    sum_sibling(1)
    wo_in.wait()
    normalize(0)
    mix_far(0)
    sum_passed(1)
    mix_plain(0, RIGHT)
    mix_plain(0, LEFT)
    mix_own(0)
    mix_passed(0)
    normalize(1)
    mix_far(1)
    mix_plain(1, RIGHT)
    mix_plain(1, LEFT)
    mix_own(1)
    mix_last(0)
    mix_passed(1)
    mix_last(1)
    left_here(xg.at[:, pl.ds(0, 3)], gs.at[0])
    left_here(kv.at[:, pl.ds(0, 3)], xs.at[0])
    left_here(qb.at[:, pl.ds(0, 3)], xs.at[1])
    left_here(oq.at[1 - c], xs.at[2])
    left_here(okv.at[1 - c], xs.at[3])
    left_here(os1, o1s.at[0])
    left_here(os2, o2s.at[0])
    left_here(oss, oqs.at[0])
    left_here(zs1, z1s.at[0])
    left_here(zs2, z2s.at[0])
    for copy in outgoing:
        copy.wait()


def per_device(tokens, w_qkv, w_out, block_perm):
    table = jnp.asarray(np.concatenate(rope_tables(block_perm.shape[0] // 8)))
    hbm = pl.BlockSpec(memory_space=pl.ANY)
    dma = pltpu.SemaphoreType.DMA
    return pl.pallas_call(
        kernel,
        name="attention_layer",
        out_shape=jax.ShapeDtypeStruct((2 * R, DW), BF),
        in_specs=[hbm] * 5,
        out_specs=hbm,
        scratch_shapes=[
            pltpu.SMEM(block_perm.shape, jnp.int32),
            pltpu.VMEM(table.shape, F32),
            pltpu.VMEM((2, N, R, DW), BF),
            pltpu.VMEM((3, N * DW, DW), BF),
            pltpu.VMEM((DW, N * DW), BF),
            pltpu.VMEM((2, R, 3 * DW), F32),
            pltpu.VMEM((2 * R, HD), F32),
            pltpu.VMEM((2 * R, HD), F32),
            pltpu.VMEM((2 * HD, 2 * HD), BF),
            pltpu.VMEM((2, 2, 2, R, HW), BF),
            pltpu.VMEM((2, 2, R, HW), BF),
            pltpu.VMEM((2, N, 2, 2, R, HW), BF),
            pltpu.VMEM((2, N, 2, R, HW), BF),
            pltpu.VMEM((2, N, 2, R, HW), F32),
            pltpu.VMEM((2, N, 2, R, HW), F32),
            pltpu.VMEM((2, 2, OB, HW), BF),
            pltpu.VMEM((2, 2, OB, HW), BF),
            pltpu.VMEM((2, 2, 2, OB, HW), BF),
            pltpu.VMEM((2, 2, 2, OB, HW), BF),
            pltpu.VMEM((2, OB, HW), BF),
            pltpu.VMEM((2, OB, HW), BF),
            pltpu.VMEM((2, 2, R, HW), BF),
            pltpu.VMEM((2, 2, R // 2, DW), BF),
            pltpu.VMEM((2, 2, R // 2, DW), BF),
            pltpu.VMEM((2, 2, R // 2, DW), F32),
            pltpu.VMEM((2, R, DW), F32),
            pltpu.VMEM((2, 2, 2, R // 2, DW), BF),
            pltpu.VMEM((2, 2, 2, R // 2, DW), BF),
            pltpu.VMEM((2, R, DW), BF),
            dma((9,)),
            dma((1,)),
            dma((3, 4)),
            dma((4,)),
            dma((3, 8)),
            dma((1,)),
            dma((2,)),
            dma((1,)),
            dma((2,)),
            dma((1,)),
            dma((2,)),
            dma((1,)),
            dma((2,)),
            dma((1,)),
            dma((2,)),
        ],
        compiler_params=pltpu.CompilerParams(
            collective_id=0, has_side_effects=True, vmem_limit_bytes=64 * 1024 * 1024 - 65536
        ),
    )(block_perm, table, tokens, w_qkv, w_out)


def solution(mesh):
    in_specs = (P("ctx", "head"), P(None, None, "head"), P("head", None), P())
    return jax.shard_map(
        per_device, mesh=mesh, in_specs=in_specs, out_specs=P("ctx", "head"), check_vma=False
    )
```
